32 devices in a mesh: dp: 4 (over y, core), seq: 8 (over z, x).
Axes of the slice: x: 2, y: 2, z: 4, core: 2. Of those that a mesh axis runs over, the one named last changes fastest.
Arguments:
- tokens: bfloat16 [32768, 2048], P(('dp', 'seq')), parts along dimension 0, may hold values from -6 to 6
- chosen: int32 [4096], P('dp'), parts along dimension 0, may hold values from 0 to 8191, as said below
- gates: float32 [4096], P('dp'), parts along dimension 0, may hold values from 0.5 to 2
- w_query: bfloat16 [2048, 1024], P('seq'), may hold values from -1.8561553 to 1.8561553
- w_key: bfloat16 [2048, 256], P('seq'), may hold values from -0.088388348 to 0.088388348
- w_value: bfloat16 [2048, 256], P('seq'), may hold values from -0.125 to 0.125
- w_out: bfloat16 [1024, 2048], P(None, 'seq'), may hold values from -0.5 to 0.5
Outputs:
- mixed: bfloat16 [32768, 2048], P(('dp', 'seq')), parts along dimension 0
The draws below stay inside these ranges and needn't reach their ends.
There are 4 independent parts, one for each index of `dp`. The reference program is written for one: setup_inputs(seed, part) draws one part's arguments, and reference() takes and returns one part's arrays. A program takes and returns all parts, laid end to end along the dimension named above; an argument that names none is the same for every part. Nothing has to cross between parts.
Inputs may be any that keep to these rules, and one draw needn't show every extreme that they name: `chosen`: distinct positions in increasing order; at most 256 of them lie in one device's 1024 consecutive positions, and exactly 256 lie in some device's positions.
All inputs are finite; a program needn't handle non-finite values.
Results may differ from the reference program's by a relative error of at most 0.006.
Values may be sent and summed in bfloat16 or wider, within the bound.
A program may use at most 128 MiB of HBM per device.

```python
import math
import jax
import jax.numpy as jnp
from jax import lax

D = 2048
HEADS = 8
KV_HEADS = 2
HEAD_DIM = 128
TOK_DEV = 1024
ROWS_DEV = 128
TOKENS = 8192
CHOSEN = 1024
N_SEQ = 8


def draw_chosen(key, part):
    lifts = jax.random.randint(jax.random.fold_in(key, 1), (N_SEQ,), 0, ROWS_DEV + 1)
    heavy = jax.random.randint(jax.random.fold_in(key, 2), (), 0, N_SEQ)
    order = jnp.arange(N_SEQ, dtype=jnp.int32)
    lifts = jnp.where(order == heavy, ROWS_DEV, lifts)
    lifts = jnp.where(order == (heavy + N_SEQ - 1) % N_SEQ, 0, lifts)
    counts = ROWS_DEV + lifts - jnp.roll(lifts, 1)
    subkeys = jax.random.split(jax.random.fold_in(key, 3), N_SEQ)
    ranks = jax.vmap(lambda single: jax.random.permutation(single, TOK_DEV))(subkeys)
    flags = (ranks < counts[:, None]).reshape(-1)
    return jnp.nonzero(flags, size=CHOSEN)[0].astype(jnp.int32)


def shared_base(key):
    raw = jax.random.normal(jax.random.fold_in(key, 11), (D, KV_HEADS * HEAD_DIM), jnp.float32)
    return jnp.clip(raw, -4.0, 4.0) * D ** (-0.5)


def draw_w_key(key, part):
    return shared_base(key).astype(jnp.bfloat16)


def draw_w_query(key, part):
    raw = jax.random.normal(jax.random.fold_in(key, 12), (D, HEADS * HEAD_DIM), jnp.float32)
    noise = jnp.clip(raw, -4.0, 4.0) * 2.0 * D ** (-0.5)
    return noise.astype(jnp.bfloat16)


def steps_of(rng, dims, cuts, least, top_value):
    gain = 1.0
    for position, shards_of in cuts:
        steps = jax.random.uniform(jax.random.fold_in(jax.random.fold_in(rng, 6), position), (shards_of,), jnp.float32, least / len(cuts), top_value / len(cuts))
        gain = gain * jnp.repeat(jnp.exp(steps), dims[position] // shards_of).reshape((-1,) + (1,) * (len(dims) - 1 - position))
    return gain


def bell_draw(rng, dims, spread, limit, cuts=(), kind=jnp.bfloat16):
    drawn = spread * jax.random.normal(rng, dims, jnp.float32)
    if cuts:
        drawn = drawn * steps_of(rng, dims, cuts, -0.22, 0.18)
    return jnp.clip(drawn, -limit, limit).astype(kind)


def setup_inputs(seed: int = 0, part: int = 0) -> dict:
    splits = jax.random.split(jax.random.key(seed), 8)
    part_splits = jax.random.split(jax.random.fold_in(splits[7], part), 8)
    return {
        "tokens": bell_draw(part_splits[0], (TOKENS, D), 1.0, 6.0, ((0, 8),)),
        "chosen": draw_chosen(jax.random.fold_in(jax.random.fold_in(splits[7], part), 71), part),
        "gates": jnp.clip(jax.random.uniform(part_splits[2], (CHOSEN,), jnp.float32, 0.5, 2.0), 0.5, 2.0),
        "w_query": draw_w_query(jax.random.fold_in(splits[7], 71), part),
        "w_key": draw_w_key(jax.random.fold_in(splits[7], 71), part),
        "w_value": bell_draw(splits[5], (D, KV_HEADS * HEAD_DIM), D ** -0.5, 0.125, ((0, 8),)),
        "w_out": bell_draw(splits[6], (HEADS * HEAD_DIM, D), (HEADS * HEAD_DIM // 9) ** -0.5, 0.5, ((1, 8),)),
    }


neg_fill = -1e+30

def reference(tokens, chosen, gates, w_query, w_key, w_value, w_out):
    picked_total = chosen.shape[0]
    group_size = HEADS // KV_HEADS
    block_rows = math.gcd(picked_total, 512)
    picked = tokens[chosen].astype(jnp.float32)
    normed = (picked * lax.rsqrt(lax.optimization_barrier(jnp.mean(picked * picked, axis=1, keepdims=True)) + 1e-06)).astype(jnp.bfloat16)
    query_matrix = (jnp.dot(normed, w_query, preferred_element_type=jnp.float32) * HEAD_DIM ** (-0.5)).astype(jnp.bfloat16)
    keys_all = jnp.dot(normed, w_key, preferred_element_type=jnp.float32).astype(jnp.bfloat16)
    values = jnp.dot(normed, w_value, preferred_element_type=jnp.float32).astype(jnp.bfloat16)
    query_matrix = lax.optimization_barrier(query_matrix).astype(jnp.float32)
    keys_expanded = lax.optimization_barrier(keys_all).astype(jnp.float32).reshape(picked_total, KV_HEADS, HEAD_DIM)
    values_expanded = lax.optimization_barrier(values).astype(jnp.float32).reshape(picked_total, KV_HEADS, HEAD_DIM)
    blocks = query_matrix.reshape(picked_total // block_rows, block_rows, KV_HEADS, group_size, HEAD_DIM)
    firsts = (jnp.arange(picked_total // block_rows, dtype=jnp.int32) * block_rows).astype(jnp.int32)
    key_order = jnp.arange(picked_total, dtype=jnp.int32)

    def one_block(inputs):
        query_tile, first_row = inputs
        logit_scores = jnp.einsum('qjfh,ujh->jfqu', query_tile, keys_expanded)
        query_order = first_row + jnp.arange(block_rows, dtype=jnp.int32)
        allowed = key_order[None, :] <= query_order[:, None]
        logit_scores = jnp.where(allowed, logit_scores, neg_fill)
        top_score = lax.optimization_barrier(jnp.max(logit_scores, axis=-1, keepdims=True))
        probs = jnp.where(allowed, jnp.exp(logit_scores - top_score), 0.0)
        totals = lax.optimization_barrier(jnp.sum(probs, axis=-1))
        softmax_weights = lax.optimization_barrier(probs.astype(jnp.bfloat16)).astype(jnp.float32)
        summed_total = jnp.einsum('yoih,hyf->yoif', softmax_weights, values_expanded)
        attended = summed_total / totals[..., None]
        return jnp.transpose(attended, (2, 0, 1, 3)).reshape(block_rows, HEADS * HEAD_DIM)
    attended = lax.map(one_block, (blocks, firsts)).reshape(picked_total, HEADS * HEAD_DIM).astype(jnp.bfloat16)
    block_out = jnp.dot(attended, w_out, preferred_element_type=jnp.float32).astype(jnp.bfloat16)
    block_wide = lax.optimization_barrier(block_out).astype(jnp.float32)
    mixed = tokens.astype(jnp.float32).at[chosen].add(gates[:, None] * block_wide)
    return mixed.astype(jnp.bfloat16)
```

```python
import functools

import jax
import jax.numpy as jnp
from jax import lax
from jax.experimental import pallas as pl
from jax.experimental.pallas import tpu as pltpu
from jax.sharding import PartitionSpec as P

HEADS = 8
KV_HEADS = 2
HEAD_DIM = 128
MOST_OWN = 256
ONES = 16
Q_SHARE = 9
O_SHARE = 9
MESH = pl.DeviceIdType.MESH
NEG = -1e30
F32 = jnp.float32
BF16 = jnp.bfloat16


class Ring:
    def __init__(self, geo, sems, region_in, region_y):
        self.g = geo
        self.sems = sems
        self.region_in = region_in
        self.region_y = region_y
        self.sends = []
        a_count, b_count = geo["A"], geo["B"]
        self.order = arrivals(a_count, b_count)

    def piece(self, k, j):
        return piece_of(self.g, k, j)

    def copy(self, kind, index, ref, dp, seq):
        send, recv = self.sems[kind]
        return remote(ref, send.at[index], recv.at[index], dp, seq)

    def send(self, *args):
        made = self.copy(*args)
        made.start()
        self.sends.append(made)

    def arrive(self, kind, index, ref):
        self.copy(kind, index, ref, self.g["dp"], self.g["z_next"]).wait_recv()

    def mine(self, s):
        return self.region_in(s, self.g["y"], self.g["c"])

    def send_core(self, k, j):
        g = self.g
        self.send("d", self.order.index((k, j)), self.mine(self.piece(k, j)), g["dp_c"], g["seq"])

    def send_y(self, k, j):
        g = self.g
        ref = self.region_y(self.piece(k, j), g["y"], g["c"])
        self.send("y", self.order.index((k, j)), ref, g["dp_y"], g["seq"])

    def slow(self, k):
        g = self.g
        s = self.piece(k, 0)
        if k > 0:
            self.arrive("z", k - 1, self.mine(s))
        if k < g["A"] - 1:
            self.send("z", k, self.mine(s), g["dp"], g["z_next"])
        if g["B"] > 1:
            self.send("x", k * (g["B"] - 1), self.mine(s), g["dp"], g["x_next"])
        if k > 0:
            self.send_core(k, 0)

    def fast(self, k, j):
        g = self.g
        s = self.piece(k, j)
        self.arrive("x", k * (g["B"] - 1) + j - 1, self.mine(s))
        if j < g["B"] - 1:
            self.send("x", k * (g["B"] - 1) + j, self.mine(s), g["dp"], g["x_next"])
        self.send_core(k, j)

    def relay(self, k, j):
        g = self.g
        index = self.order.index((k, j))
        ref = self.region_y(self.piece(k, j), 1 - g["y"], g["c"])
        self.arrive("y", index, ref)
        self.send("d", len(self.order) + index, ref, g["dp_c"], g["seq"])

    def from_core(self, k, j):
        g = self.g
        index = self.order.index((k, j))
        s = self.piece(k, j)
        self.arrive("d", index, self.region_in(s, g["y"], 1 - g["c"]))
        self.arrive("d", len(self.order) + index, self.region_y(s, 1 - g["y"], 1 - g["c"]))

    def finish(self):
        for made in self.sends:
            made.wait_send()


class Causal:
    def __init__(self, geo, sems, ref, parts):
        self.g = geo
        self.sems = sems
        self.ref = ref
        self.parts = parts
        self.sends = []

    def has(self, k, j):
        g = self.g
        if k > 0:
            return g["a"] >= k
        return g["b"] >= j

    def copy(self, kind, index, e, s, seq):
        send, recv = self.sems[kind]
        at = index * self.parts + e
        return remote(self.ref(s, e), send.at[at], recv.at[at], self.g["dp"], seq)

    def send(self, cond, *args):
        made = self.copy(*args)
        pl.when(cond)(made.start)
        self.sends.append((cond, made))

    def arrive(self, cond, *args):
        pl.when(cond)(self.copy(*args, self.g["z_next"]).wait_recv)

    def slow(self, k):
        g = self.g
        s = piece_of(g, k, 0)
        for e in range(self.parts):
            if k > 0:
                self.arrive(g["a"] >= k, "z", k - 1, e, s)
            if k < g["A"] - 1:
                cond = jnp.logical_and(g["a"] >= k, g["a"] + 1 < g["A"])
                self.send(cond, "z", k, e, s, g["z_next"])
            if g["B"] > 1:
                cond = g["a"] >= k if k > 0 else g["b"] + 1 < g["B"]
                self.send(cond, "x", k * (g["B"] - 1), e, s, g["x_next"])

    def fast(self, k, j):
        g = self.g
        s = piece_of(g, k, j)
        for e in range(self.parts):
            self.arrive(self.has(k, j), "x", k * (g["B"] - 1) + j - 1, e, s)
            if j < g["B"] - 1:
                cond = self.has(k, j)
                if k == 0:
                    cond = jnp.logical_and(cond, g["b"] + 1 < g["B"])
                self.send(cond, "x", k * (g["B"] - 1) + j, e, s, g["x_next"])

    def finish(self):
        for cond, made in self.sends:
            pl.when(cond)(made.wait_send)


def remote(ref, send, recv, dp, seq):
    return pltpu.make_async_remote_copy(
        src_ref=ref,
        dst_ref=ref,
        send_sem=send,
        recv_sem=recv,
        device_id=(dp, seq),
        device_id_type=MESH,
    )


def arrivals(a_count, b_count):
    order = []
    for k in range(1, a_count):
        order += [(k, 0)] + [(k - 1, j) for j in range(1, b_count)]
    return order + [(a_count - 1, j) for j in range(1, b_count)]


def piece_of(g, k, j):
    a = lax.rem(g["a"] - k + g["A"], g["A"])
    b = lax.rem(g["b"] - j + g["B"], g["B"])
    return a * g["B"] + b


def up16(value):
    return (value + 15) // 16 * 16


def main_kernel(
    A, B, tok, ch, wq, wk, wv, wo, blk, oh_out,
    tok_v, kvw, qw, obuf, kv, normed, qt, acc, m_s, counts, att, lsem,
    wz, wx, wy, wd, qz, qx, qy, qd, oz, ox, oy, od, kz, kx,
):
    n = A * B
    dp = lax.axis_index("dp")
    seq = lax.axis_index("seq")
    a, b = seq // B, lax.rem(seq, B)
    y, c = lax.rem(dp // 2, 2), lax.rem(dp, 2)
    z_next = lax.rem(a + 1, A) * B + b
    z_prev = lax.rem(a + A - 1, A) * B + b
    x_next = a * B + lax.rem(b + 1, B)
    x_prev = a * B + lax.rem(b + B - 1, B)
    dp_y = dp + 2 * (1 - 2 * y)
    dp_c = dp + 1 - 2 * c
    geo = dict(
        A=A, B=B, a=a, b=b, y=y, c=c, dp=dp, seq=seq,
        z_next=z_next, x_next=x_next, dp_y=dp_y, dp_c=dp_c,
    )
    t_rows = tok.shape[0]
    width = tok.shape[1]
    k_rows = wq.shape[0]
    q_cols, e_cols = wq.shape[1], wk.shape[1]
    o_rows, o_cols = wo.shape
    group = HEADS // KV_HEADS
    pair = 2 * HEAD_DIM

    rows_here = pl.ds(pl.multiple_of(seq * k_rows, k_rows), k_rows)
    local = []
    for e in range(KV_HEADS):
        cols = pl.ds(e * HEAD_DIM, HEAD_DIM)
        local.append((wk.at[:, cols], kvw.at[rows_here, pl.ds(e * pair, HEAD_DIM)]))
        local.append((wv.at[:, cols], kvw.at[rows_here, pl.ds(e * pair + HEAD_DIM, HEAD_DIM)]))
    local += [(wq, qw.at[rows_here, :]), (tok, tok_v), (wo, obuf.at[seq])]
    local = [pltpu.make_async_copy(s, d, lsem.at[i]) for i, (s, d) in enumerate(local)]
    for made in local:
        made.start()
    load_kv, (load_q, load_tok, load_o) = local[: 2 * KV_HEADS], local[2 * KV_HEADS :]

    greet = [(dp, z_next)] + ([(dp, z_prev)] if A > 2 else [])
    if B > 1:
        greet += [(dp, x_next)] + ([(dp, x_prev)] if B > 2 else [])
    greet += [(dp_y, seq), (dp_c, seq)]
    barrier = pltpu.get_barrier_semaphore()
    for who in greet:
        pl.semaphore_signal(barrier, inc=1, device_id=who, device_id_type=MESH)
    pl.semaphore_wait(barrier, len(greet))

    quarter = 2 * e_cols // 4

    def w_region(s, y, c):
        return kvw.at[
            pl.ds(pl.multiple_of(s * k_rows, k_rows), k_rows),
            pl.ds(pl.multiple_of((2 * c + y) * quarter, 128), quarter),
        ]

    q_half = q_cols // 2
    q_in = up16(k_rows * Q_SHARE // 16)

    def q_region(s, c, start, size):
        return qw.at[
            pl.ds(pl.multiple_of(s * k_rows + start, 16), size),
            pl.ds(pl.multiple_of(c * q_half, 128), q_half),
        ]

    o_half = o_rows // 2
    o_in = up16(o_half * O_SHARE // 16)

    def o_region(s, start, size):
        return obuf.at[s, pl.ds(pl.multiple_of(start, 16), size), :]

    W = Ring(geo, {"z": wz, "x": wx, "y": wy, "d": wd}, w_region, w_region)
    Q = Ring(
        geo,
        {"z": qz, "x": qx, "y": qy, "d": qd},
        lambda s, y, c: q_region(s, c, y * (k_rows - q_in), q_in),
        lambda s, y, c: q_region(s, c, y * q_in, k_rows - q_in),
    )
    O = Ring(
        geo,
        {"z": oz, "x": ox, "y": oy, "d": od},
        lambda s, y, c: o_region(s, c * o_half + y * (o_half - o_in), o_in),
        lambda s, y, c: o_region(s, c * o_half + y * o_in, o_half - o_in),
    )
    K = Causal(geo, {"z": kz, "x": kx}, lambda s, e: kv.at[s, e], KV_HEADS)
    order = W.order

    for made in load_kv:
        made.wait()
    W.slow(0)
    load_q.wait()
    Q.slow(0)

    def gather():
        base = seq * t_rows
        picks = ch[...]
        start = jnp.sum((picks < base).astype(F32), axis=1, keepdims=True)
        rel = picks - base
        inside = (rel >= 0) & (rel < t_rows)
        place = jnp.where(inside, (rel + 1).astype(F32), 0.0)
        rank = lax.broadcasted_iota(jnp.int32, picks.shape, 1).astype(F32) - start
        slots = lax.broadcasted_iota(jnp.int32, (MOST_OWN, 1), 0).astype(F32)
        own = jnp.sum(jnp.where(rank == slots, place, 0.0), axis=1, keepdims=True) - 1.0
        spots = lax.broadcasted_iota(jnp.int32, (1, t_rows), 1).astype(F32)
        oh_out[...] = (own == spots).astype(F32).astype(BF16)
        for t in range(n):
            held = (picks >= t * t_rows) & (picks < (t + 1) * t_rows)
            count = jnp.sum(held.astype(F32), axis=1, keepdims=True)
            counts[t] = jnp.broadcast_to(count, (1, HEAD_DIM))
        load_tok.wait()
        chunk = 512
        square = jnp.zeros((MOST_OWN, 1), F32)
        for i in range(width // chunk):
            cols = slice(i * chunk, (i + 1) * chunk)
            rows = jnp.dot(oh_out[...], tok_v[:, cols], preferred_element_type=F32)
            square = square + jnp.sum(rows * rows, axis=1, keepdims=True)
            normed[:, cols] = rows.astype(BF16)
        scale = lax.rsqrt(square / width + 1e-06)
        for i in range(width // chunk):
            cols = slice(i * chunk, (i + 1) * chunk)
            normed[:, cols] = (normed[:, cols].astype(F32) * scale).astype(BF16)

    def project_kv():
        for e in range(KV_HEADS):
            part = jnp.dot(
                normed[...], kvw[:, e * pair : (e + 1) * pair], preferred_element_type=F32
            )
            kv[seq, e, 0] = part[:, :HEAD_DIM].astype(BF16)
            flip = part[:, HEAD_DIM:].T.astype(BF16)
            kv[seq, e, 1, :HEAD_DIM, :] = flip[:, :HEAD_DIM]
            kv[seq, e, 1, HEAD_DIM:, :] = flip[:, HEAD_DIM:]

    def project_q():
        for i in range(HEADS // 2):
            part = jnp.dot(
                normed[...], qw[:, i * pair : (i + 1) * pair], preferred_element_type=F32
            )
            part = part * HEAD_DIM**-0.5
            for h in range(2):
                head = i * 2 + h
                e, first = head // group, (head % group) * MOST_OWN
                flip = part[:, h * HEAD_DIM : (h + 1) * HEAD_DIM].T.astype(BF16)
                qt[e, :HEAD_DIM, first : first + MOST_OWN] = flip
        row = lax.broadcasted_iota(jnp.int32, (HEAD_DIM, group * MOST_OWN), 0)
        for e in range(KV_HEADS):
            qt[e, HEAD_DIM:, :] = (row == 0).astype(F32).astype(BF16)

    def attend(t, diagonal):
        row = lax.broadcasted_iota(jnp.int32, (MOST_OWN, HEAD_DIM), 0).astype(F32)
        bias = jnp.where(row < counts[t], 0.0, NEG).astype(BF16)
        ones = jnp.ones((ONES, MOST_OWN), BF16)
        heads = range(HEADS)
        left, right = [], []
        for e in range(KV_HEADS):
            left.append(jnp.concatenate([kv[t, e, 0], bias], axis=1))
            flip = [kv[t, e, 1, :HEAD_DIM, :], kv[t, e, 1, HEAD_DIM:, :]]
            right.append(jnp.concatenate([jnp.concatenate(flip, axis=1), ones], axis=0))
        score = []
        for f in heads:
            first = (f % group) * MOST_OWN
            query = qt[f // group, :, first : first + MOST_OWN]
            score.append(jnp.dot(left[f // group], query, preferred_element_type=F32))
        if diagonal:
            key = lax.broadcasted_iota(jnp.int32, (MOST_OWN, MOST_OWN), 0)
            asks = lax.broadcasted_iota(jnp.int32, (MOST_OWN, MOST_OWN), 1)
            score = [jnp.where(key <= asks, s, NEG) for s in score]
            top = [jnp.max(s, axis=0, keepdims=True) for s in score]
        else:
            old = [m_s[f] for f in heads]
            held = [acc[f] for f in heads]
            top = [
                jnp.maximum(o, jnp.max(s, axis=0, keepdims=True)) for o, s in zip(old, score)
            ]
        prob = [jnp.exp(s - m).astype(BF16) for s, m in zip(score, top)]
        new = [
            jnp.dot(right[f // group], prob[f], preferred_element_type=F32) for f in heads
        ]
        if not diagonal:
            new = [h * jnp.exp(o - m) + v for h, o, m, v in zip(held, old, top, new)]
        for f in heads:
            m_s[f] = top[f]
            acc[f] = new[f]

    def attend_past(k, j):
        pl.when(K.has(k, j))(lambda: attend(piece_of(geo, k, j), False))

    waiting = []

    def pump(count):
        for _ in range(min(count, len(waiting))):
            ring, k, j = waiting.pop(0)
            ring.send_y(k, j)

    def step(ring, k):
        got = []
        if k < A:
            ring.slow(k)
            got.append((k, 0))
        for j in range(1, B):
            ring.fast(k - 1, j)
            got.append((k - 1, j))
        waiting.extend((ring, *kj) for kj in got)
        return got

    gather()
    before = []
    for k in range(1, A + 1):
        kept, waiting[:] = waiting[:], []
        got = step(W, k)
        pump(len(got))
        waiting.extend(kept)
        for kj in before:
            W.relay(*kj)
        before = got
        step(Q, k)
        if k < A:
            pump(1)
        if k == max(A - 1, 1):
            load_o.wait()
            O.slow(0)
    pump(len(waiting))
    for kj in before:
        W.relay(*kj)
    for kj in order:
        W.from_core(*kj)
    project_kv()
    K.slow(0)
    step(O, 1)
    pump(len(waiting))
    if A > 1:
        K.slow(1)
    for j in range(1, B):
        K.fast(0, j)
    if A > 1:
        step(O, 2)
        pump(len(waiting))
    for kj in order:
        Q.relay(*kj)
    for kj in order:
        Q.from_core(*kj)
    project_q()
    attend(seq, True)
    for k in range(1, A):
        if k + 1 < A:
            K.slow(k + 1)
        for j in range(1, B):
            K.fast(k, j)
        attend_past(k, 0)
        for j in range(1, B):
            attend_past(k - 1, j)
        if k + 2 <= A:
            step(O, k + 2)
            pump(len(waiting))
    for j in range(1, B):
        attend_past(A - 1, j)
    for kj in order:
        O.relay(*kj)
    for f in range(HEADS):
        total = acc[f]
        flip = (total[:HEAD_DIM] / total[HEAD_DIM : HEAD_DIM + 1]).T
        att[:, f * HEAD_DIM : (f + 1) * HEAD_DIM] = flip.astype(BF16)

    def project_out(s):
        cols = pl.ds(pl.multiple_of(s * o_cols, o_cols), o_cols)
        blk[:, cols] = jnp.dot(att[...], obuf[s], preferred_element_type=F32).astype(BF16)

    if o_cols % 128 == 0:
        project_out(seq)
    for kj in order:
        O.from_core(*kj)
        if o_cols % 128 == 0:
            project_out(piece_of(geo, *kj))
    if o_cols % 128 != 0:
        for s in range(n):
            blk[:, s * o_cols : (s + 1) * o_cols] = jnp.dot(
                att[...], obuf[s], preferred_element_type=F32
            ).astype(BF16)
    for ring in (W, Q, O, K):
        ring.finish()


def add_kernel(tile, tok, ch, gates, oh, blk, out):
    seq = lax.axis_index("seq")
    t_rows = tile * pl.num_programs(0)
    low = seq * t_rows + pl.program_id(0) * tile
    rows = lax.broadcasted_iota(jnp.int32, (tile, 1), 0) + low
    gate = jnp.sum(jnp.where(ch[...] == rows, gates[...], 0.0), axis=1, keepdims=True)
    lift = lax.dot_general(
        oh[...], blk[...], (((0,), (0,)), ((), ())), preferred_element_type=F32
    )
    out[...] = (tok[...].astype(F32) + gate * lift).astype(BF16)


def per_device(tokens, chosen, gates, w_query, w_key, w_value, w_out):
    n = lax.axis_size("seq")
    A = 4 if n % 4 == 0 else 1
    B = n // A
    t_rows, width = tokens.shape
    k_rows, q_cols = w_query.shape
    e_cols = w_key.shape[1]
    o_rows, o_cols = w_out.shape
    picks = chosen.reshape(1, -1)
    gate_row = gates.reshape(1, -1)
    dma = pltpu.SemaphoreType.DMA
    any_spec = pl.BlockSpec(memory_space=pl.ANY)
    vmem_spec = pl.BlockSpec(memory_space=pltpu.VMEM)
    steps_x = max(A * (B - 1), 1)
    steps_z = max(A - 1, 1)

    def pair(count):
        return (dma((count,)), dma((count,)))

    sems = []
    for _ in range(3):
        sems += [pair(steps_z), pair(steps_x), pair(n - 1), pair(2 * (n - 1))]
    sems += [pair(KV_HEADS * steps_z), pair(KV_HEADS * steps_x)]
    flat = [x for two in sems for x in two]

    def body(*refs):
        head, tail = refs[: len(refs) - len(flat)], refs[len(refs) - len(flat) :]
        pairs = [(tail[i], tail[i + 1]) for i in range(0, len(tail), 2)]
        main_kernel(A, B, *head, *pairs)

    blk, oh = pl.pallas_call(
        body,
        out_shape=(
            jax.ShapeDtypeStruct((MOST_OWN, width), BF16),
            jax.ShapeDtypeStruct((MOST_OWN, t_rows), BF16),
        ),
        in_specs=[any_spec, vmem_spec] + [any_spec] * 4,
        out_specs=(vmem_spec, vmem_spec),
        scratch_shapes=[
            pltpu.VMEM((t_rows, width), BF16),
            pltpu.VMEM((n * k_rows, 2 * e_cols), BF16),
            pltpu.VMEM((n * k_rows, q_cols), BF16),
            pltpu.VMEM((n, o_rows, o_cols), BF16),
            pltpu.VMEM((n, KV_HEADS, 2, MOST_OWN, HEAD_DIM), BF16),
            pltpu.VMEM((MOST_OWN, width), BF16),
            pltpu.VMEM((KV_HEADS, 2 * HEAD_DIM, HEADS // KV_HEADS * MOST_OWN), BF16),
            pltpu.VMEM((HEADS, HEAD_DIM + ONES, MOST_OWN), F32),
            pltpu.VMEM((HEADS, 1, MOST_OWN), F32),
            pltpu.VMEM((n, 1, HEAD_DIM), F32),
            pltpu.VMEM((MOST_OWN, HEADS * HEAD_DIM), BF16),
            dma((2 * KV_HEADS + 3,)),
            *flat,
        ],
        compiler_params=pltpu.CompilerParams(
            collective_id=0, has_side_effects=True, vmem_limit_bytes=60 * 1024 * 1024
        ),
        name="gather_attend",
    )(tokens, picks, w_query, w_key, w_value, w_out)

    tile = 256
    return pl.pallas_call(
        functools.partial(add_kernel, tile),
        grid=(t_rows // tile,),
        out_shape=jax.ShapeDtypeStruct((t_rows, width), BF16),
        in_specs=[
            pl.BlockSpec((tile, width), lambda i: (i, 0)),
            pl.BlockSpec(picks.shape, lambda i: (0, 0)),
            pl.BlockSpec(picks.shape, lambda i: (0, 0)),
            pl.BlockSpec((MOST_OWN, tile), lambda i: (0, i)),
            pl.BlockSpec((MOST_OWN, width), lambda i: (0, 0)),
        ],
        out_specs=pl.BlockSpec((tile, width), lambda i: (i, 0)),
        compiler_params=pltpu.CompilerParams(vmem_limit_bytes=62 * 1024 * 1024),
        name="add_rows",
    )(tokens, picks, gate_row, oh, blk)


def solution(mesh):
    return jax.shard_map(
        per_device,
        mesh=mesh,
        in_specs=(
            P(("dp", "seq"), None),
            P("dp"),
            P("dp"),
            P("seq", None),
            P("seq", None),
            P("seq", None),
            P(None, "seq"),
        ),
        out_specs=P(("dp", "seq"), None),
        check_vma=False,
    )
```

```python
import functools

import jax
import jax.numpy as jnp
from jax import lax
from jax.experimental import pallas as pl
from jax.experimental.pallas import tpu as pltpu
from jax.sharding import PartitionSpec as P

HEADS = 8
KV_HEADS = 2
HEAD_DIM = 128
MOST_OWN = 256
ONES = 16
TILES = 4
ADD_TILES = 4
MAIN_VMEM = 36
ADD_VMEM = 12
Q_SHARE = 9
O_SHARE = 17
PLAN = (
    ("W", "oz", 0, 0), ("Q", "ox", 0, 0), ("W", "ox", 0, 0), ("Q", "oz", 0, 0), ("gather",),
    ("W", "z", 1, 0), ("W", "ys", 1, 0), ("O", "ox", 0, 0), ("gates", 0), ("Q", "x", 0, 1),
    ("Q", "ys", 0, 1), ("Q", "z", 1, 0), ("gates", 1), ("Q", "ys", 1, 0), ("W", "x", 1, 1),
    ("W", "z", 2, 0), ("gates", 2), ("W", "ys", 2, 0), ("O", "oz", 0, 0), ("W", "ys", 1, 1),
    ("gates", 3), ("W", "x", 0, 1), ("W", "ys", 0, 1), ("W", "y", 1, 0), ("W", "z", 3, 0),
    ("Q", "z", 2, 0), ("W", "ys", 3, 0), ("W", "x", 2, 1), ("W", "ys", 2, 1), ("Q", "y", 0, 1),
    ("Q", "ys", 2, 0), ("W", "y", 0, 1), ("O", "x", 0, 1), ("O", "z", 1, 0), ("W", "x", 3, 1),
    ("W", "y", 3, 0), ("Q", "x", 1, 1), ("W", "e", 0, 1), ("Q", "y", 1, 0), ("W", "ys", 3, 1),
    ("Q", "z", 3, 0), ("W", "y", 2, 0), ("W", "y", 1, 1), ("Q", "ys", 1, 1), ("W", "y", 2, 1),
    ("W", "e", 1, 0), ("W", "e", 3, 0), ("Q", "ys", 3, 0), ("Q", "x", 2, 1), ("O", "z", 2, 0),
    ("W", "y", 3, 1), ("W", "e", 2, 1), ("O", "ys", 2, 0), ("W", "e", 2, 0), ("W", "e", 1, 1),
    ("W", "e", 3, 1), ("kv",), ("K", "z", 0, 0, 1), ("Q", "x", 3, 1), ("K", "z", 0, 0, 0),
    ("Q", "ys", 3, 1), ("Q", "ys", 2, 1), ("Q", "e", 0, 1), ("Q", "e", 1, 0), ("O", "z", 3, 0),
    ("Q", "y", 1, 1), ("Q", "y", 2, 0), ("O", "ys", 1, 0), ("K", "z", 1, 0, 1), ("O", "x", 2, 1),
    ("K", "z", 1, 0, 0), ("Q", "y", 2, 1), ("O", "ys", 0, 1), ("Q", "y", 3, 0), ("O", "ys", 3, 0),
    ("O", "ys", 2, 1), ("K", "z", 2, 0, 1), ("Q", "y", 3, 1), ("O", "y", 2, 0), ("O", "x", 1, 1),
    ("O", "x", 3, 1), ("Q", "e", 1, 1), ("Q", "e", 2, 0), ("Q", "e", 3, 0), ("Q", "e", 2, 1),
    ("Q", "e", 3, 1), ("K", "z", 2, 0, 0), ("O", "y", 1, 0), ("q",), ("K", "x", 0, 1, 1),
    ("O", "e", 2, 0), ("O", "y", 0, 1), ("O", "ys", 3, 1), ("O", "e", 1, 0), ("O", "ys", 1, 1),
    ("K", "z", 3, 0, 1), ("K", "x", 0, 1, 0), ("own",), ("O", "e", 0, 1), ("att", 1, 0),
    ("K", "x", 2, 1, 1), ("O", "y", 3, 0), ("K", "z", 3, 0, 0), ("att", 3, 0), ("att", 0, 1),
    ("O", "y", 2, 1), ("K", "x", 3, 1, 1), ("att", 2, 0), ("K", "x", 2, 1, 0), ("att", 2, 1),
    ("K", "x", 1, 1, 1), ("O", "y", 3, 1), ("O", "e", 3, 0), ("O", "e", 2, 1), ("K", "x", 3, 1, 0),
    ("att", 3, 1), ("K", "x", 1, 1, 0), ("att", 1, 1), ("norm",), ("out", 0, 0), ("out", 2, 1),
    ("O", "y", 1, 1), ("out", 3, 0), ("out", 0, 1), ("O", "e", 3, 1), ("out", 3, 1), ("out", 2, 0),
    ("out", 1, 0), ("O", "e", 1, 1), ("out", 1, 1),
)
MESH = pl.DeviceIdType.MESH
NEG = -1e30
F32 = jnp.float32
BF16 = jnp.bfloat16


class Ring:
    def __init__(self, geo, sems, region_in, region_y):
        self.g = geo
        self.sems = sems
        self.region_in = region_in
        self.region_y = region_y
        self.sends = []
        a_count, b_count = geo["A"], geo["B"]
        self.order = arrivals(a_count, b_count)

    def piece(self, k, j):
        return piece_of(self.g, k, j)

    def copy(self, kind, index, ref, dp, seq):
        send, recv = self.sems[kind]
        return remote(ref, send.at[index], recv.at[index], dp, seq)

    def send(self, *args):
        made = self.copy(*args)
        made.start()
        self.sends.append(made)

    def arrive(self, kind, index, ref):
        self.copy(kind, index, ref, self.g["dp"], self.g["z_next"]).wait_recv()

    def mine(self, s):
        return self.region_in(s, self.g["y"], self.g["c"])

    def send_core(self, k, j):
        g = self.g
        self.send("d", self.order.index((k, j)), self.mine(self.piece(k, j)), g["dp_c"], g["seq"])

    def send_y(self, k, j):
        g = self.g
        ref = self.region_y(self.piece(k, j), g["y"], g["c"])
        self.send("y", self.order.index((k, j)), ref, g["dp_y"], g["seq"])

    def send_z(self, k):
        g = self.g
        if k < g["A"] - 1:
            self.send("z", k, self.mine(self.piece(k, 0)), g["dp"], g["z_next"])

    def send_x(self, k):
        g = self.g
        if g["B"] > 1:
            ref = self.mine(self.piece(k, 0))
            self.send("x", k * (g["B"] - 1), ref, g["dp"], g["x_next"])

    def slow(self, k):
        self.arrive("z", k - 1, self.mine(self.piece(k, 0)))
        self.send_z(k)
        self.send_x(k)
        self.send_core(k, 0)

    def fast(self, k, j):
        g = self.g
        s = self.piece(k, j)
        self.arrive("x", k * (g["B"] - 1) + j - 1, self.mine(s))
        if j < g["B"] - 1:
            self.send("x", k * (g["B"] - 1) + j, self.mine(s), g["dp"], g["x_next"])
        self.send_core(k, j)

    def relay(self, k, j):
        g = self.g
        index = self.order.index((k, j))
        ref = self.region_y(self.piece(k, j), 1 - g["y"], g["c"])
        self.arrive("y", index, ref)
        self.send("d", len(self.order) + index, ref, g["dp_c"], g["seq"])

    def from_core(self, k, j):
        g = self.g
        index = self.order.index((k, j))
        s = self.piece(k, j)
        self.arrive("d", index, self.region_in(s, g["y"], 1 - g["c"]))
        self.arrive("d", len(self.order) + index, self.region_y(s, 1 - g["y"], 1 - g["c"]))

    def finish(self):
        for made in self.sends:
            made.wait_send()


class Causal:
    def __init__(self, geo, sems, ref, parts):
        self.g = geo
        self.sems = sems
        self.ref = ref
        self.parts = parts
        self.sends = []
        self.detour = geo["B"] == 2 and geo["A"] >= 2
        self.last = geo["a"] == geo["A"] - 1

    def has(self, k, j):
        g = self.g
        if k > 0:
            return g["a"] >= k
        return g["b"] >= j

    def copy(self, kind, index, e, s, seq):
        send, recv = self.sems[kind]
        at = index * self.parts + e
        return remote(self.ref(s, e), send.at[at], recv.at[at], self.g["dp"], seq)

    def send(self, cond, *args):
        made = self.copy(*args)
        pl.when(cond)(made.start)
        self.sends.append((cond, made))

    def arrive(self, cond, *args):
        pl.when(cond)(self.copy(*args, self.g["z_next"]).wait_recv)

    def slow(self, k, e):
        g = self.g
        s = piece_of(g, k, 0)
        if k > 0:
            self.arrive(g["a"] >= k, "z", k - 1, e, s)
        if k < g["A"] - 1:
            cond = jnp.logical_and(g["a"] >= k, g["a"] + 1 < g["A"])
            self.send(cond, "z", k, e, s, g["z_next"])
        if g["B"] > 1:
            cond = g["a"] >= k if k > 0 else g["b"] + 1 < g["B"]
            if self.detour and k == 1:
                turned = jnp.logical_and(self.last, g["b"] == 0)
                cond = jnp.logical_and(cond, jnp.logical_not(turned))
            self.send(cond, "x", k * (g["B"] - 1), e, s, g["x_next"])

    def fast(self, k, j, e):
        g = self.g
        s = piece_of(g, k, j)
        index = k * (g["B"] - 1) + j - 1
        has = self.has(k, j)
        if self.detour and k == 1:
            turned = jnp.logical_and(self.last, g["b"] == 1)
            self.arrive(turned, "t", 0, e, s)
            has = jnp.logical_and(has, jnp.logical_not(turned))
        self.arrive(has, "x", index, e, s)
        if self.detour and k == 0:
            cond = jnp.logical_and(g["a"] == g["A"] - 2, g["b"] == 1)
            self.send(cond, "t", 0, e, s, g["z_next"])
        if j < g["B"] - 1:
            cond = self.has(k, j)
            if k == 0:
                cond = jnp.logical_and(cond, g["b"] + 1 < g["B"])
            self.send(cond, "x", index + 1, e, s, g["x_next"])

    def finish(self):
        for cond, made in self.sends:
            pl.when(cond)(made.wait_send)


def remote(ref, send, recv, dp, seq):
    return pltpu.make_async_remote_copy(
        src_ref=ref,
        dst_ref=ref,
        send_sem=send,
        recv_sem=recv,
        device_id=(dp, seq),
        device_id_type=MESH,
    )


def arrivals(a_count, b_count):
    order = []
    for k in range(1, a_count):
        order += [(k, 0)] + [(k - 1, j) for j in range(1, b_count)]
    return order + [(a_count - 1, j) for j in range(1, b_count)]


def piece_of(g, k, j):
    a = lax.rem(g["a"] - k + g["A"], g["A"])
    b = lax.rem(g["b"] - j + g["B"], g["B"])
    return a * g["B"] + b


def plan_of(A, B):
    if (A, B) == (4, 2):
        return PLAN
    order = arrivals(A, B)
    taken = {kj: ("z" if kj[1] == 0 else "x", *kj) for kj in order}
    parts = range(KV_HEADS)
    plan = [("W", "oz", 0, 0), ("W", "ox", 0, 0), ("Q", "oz", 0, 0), ("Q", "ox", 0, 0), ("gather",)]
    for what in "WQ":
        for kj in order:
            plan += [(what, *taken[kj]), (what, "ys", *kj)]
    plan += [("O", "oz", 0, 0), ("O", "ox", 0, 0)]
    plan += [("W", "y", *kj) for kj in order] + [("W", "e", *kj) for kj in order]
    plan += [("gates", i) for i in range(TILES)] + [("kv",)] + [("K", "z", 0, 0, e) for e in parts]
    for kj in order[: len(order) // 2]:
        plan += [("O", *taken[kj]), ("O", "ys", *kj)]
    plan += [("Q", "y", *kj) for kj in order] + [("Q", "e", *kj) for kj in order]
    plan += [("q",), ("own",)]
    for i, kj in enumerate(order):
        plan += [("K", *taken[kj], e) for e in parts] + [("att", *kj)]
        if i >= len(order) // 2:
            plan += [("O", *taken[kj]), ("O", "ys", *kj)]
    plan += [("O", "y", *kj) for kj in order] + [("norm",), ("out", 0, 0)]
    for kj in order:
        plan += [("O", "e", *kj), ("out", *kj)]
    return plan


def up16(value):
    return (value + 15) // 16 * 16


def main_kernel(
    A, B, tok, ch_in, gates_in, wq, wk, wv, wo, blk, oh_out, gate_out,
    ch, gates, oh, tok_v, kvw, qw, obuf, kv, normed, qt, acc, m_s, counts, att, lsem,
    wz, wx, wy, wd, qz, qx, qy, qd, oz, ox, oy, od, kz, kx, kt,
):
    n = A * B
    dp = lax.axis_index("dp")
    seq = lax.axis_index("seq")
    a, b = seq // B, lax.rem(seq, B)
    y, c = lax.rem(dp // 2, 2), lax.rem(dp, 2)
    z_next = lax.rem(a + 1, A) * B + b
    z_prev = lax.rem(a + A - 1, A) * B + b
    x_next = a * B + lax.rem(b + 1, B)
    x_prev = a * B + lax.rem(b + B - 1, B)
    dp_y = dp + 2 * (1 - 2 * y)
    dp_c = dp + 1 - 2 * c
    geo = dict(
        A=A, B=B, a=a, b=b, y=y, c=c, dp=dp, seq=seq,
        z_next=z_next, x_next=x_next, dp_y=dp_y, dp_c=dp_c,
    )
    t_rows = tok.shape[0]
    width = tok.shape[1]
    k_rows = wq.shape[0]
    q_cols, e_cols = wq.shape[1], wk.shape[1]
    o_rows, o_cols = wo.shape
    group = HEADS // KV_HEADS
    pair = 2 * HEAD_DIM

    rows_here = pl.ds(pl.multiple_of(seq * k_rows, k_rows), k_rows)
    local = []
    for e in range(KV_HEADS):
        cols = pl.ds(e * HEAD_DIM, HEAD_DIM)
        local.append((wk.at[:, cols], kvw.at[rows_here, pl.ds(e * pair, HEAD_DIM)]))
        local.append((wv.at[:, cols], kvw.at[rows_here, pl.ds(e * pair + HEAD_DIM, HEAD_DIM)]))
    local += [(wq, qw.at[rows_here, :]), (ch_in, ch), (tok, tok_v), (wo, obuf.at[seq])]
    local += [(gates_in, gates)]
    local = [pltpu.make_async_copy(s, d, lsem.at[i]) for i, (s, d) in enumerate(local)]
    for made in local:
        made.start()
    load_kv, rest = local[: 2 * KV_HEADS], local[2 * KV_HEADS :]
    load_q, load_ch, load_tok, load_o, load_gates = rest

    greet = [(dp, z_next)] + ([(dp, z_prev)] if A > 2 else [])
    if B > 1:
        greet += [(dp, x_next)] + ([(dp, x_prev)] if B > 2 else [])
    greet += [(dp_y, seq), (dp_c, seq)]
    barrier = pltpu.get_barrier_semaphore()
    for who in greet:
        pl.semaphore_signal(barrier, inc=1, device_id=who, device_id_type=MESH)
    pl.semaphore_wait(barrier, len(greet))

    quarter = 2 * e_cols // 4

    def w_region(s, y, c):
        return kvw.at[
            pl.ds(pl.multiple_of(s * k_rows, k_rows), k_rows),
            pl.ds(pl.multiple_of((2 * c + y) * quarter, 128), quarter),
        ]

    q_half = q_cols // 2
    q_in = up16(k_rows * Q_SHARE // 16)

    def q_region(s, c, start, size):
        return qw.at[
            pl.ds(pl.multiple_of(s * k_rows + start, 16), size),
            pl.ds(pl.multiple_of(c * q_half, 128), q_half),
        ]

    o_half = o_rows // 2
    o_in = up16(o_half * O_SHARE // 32)

    def o_region(s, start, size):
        return obuf.at[s, pl.ds(pl.multiple_of(start, 16), size), :]

    W = Ring(geo, {"z": wz, "x": wx, "y": wy, "d": wd}, w_region, w_region)
    Q = Ring(
        geo,
        {"z": qz, "x": qx, "y": qy, "d": qd},
        lambda s, y, c: q_region(s, c, y * (k_rows - q_in), q_in),
        lambda s, y, c: q_region(s, c, y * q_in, k_rows - q_in),
    )
    O = Ring(
        geo,
        {"z": oz, "x": ox, "y": oy, "d": od},
        lambda s, y, c: o_region(s, c * o_half + y * (o_half - o_in), o_in),
        lambda s, y, c: o_region(s, c * o_half + y * o_in, o_half - o_in),
    )
    K = Causal(geo, {"z": kz, "x": kx, "t": kt}, lambda s, e: kv.at[s, e], KV_HEADS)

    rings = {"W": W, "Q": Q, "O": O}
    loads = {"W": load_kv, "Q": [load_q], "O": [load_o]}

    def gather():
        load_ch.wait()
        load_gates.wait()
        base = seq * t_rows
        picks = ch[...]
        start = jnp.sum((picks < base).astype(F32), axis=1, keepdims=True)
        rel = picks - base
        inside = (rel >= 0) & (rel < t_rows)
        place = jnp.where(inside, (rel + 1).astype(F32), 0.0)
        rank = lax.broadcasted_iota(jnp.int32, picks.shape, 1).astype(F32) - start
        slots = lax.broadcasted_iota(jnp.int32, (MOST_OWN, 1), 0).astype(F32)
        own = jnp.sum(jnp.where(rank == slots, place, 0.0), axis=1, keepdims=True) - 1.0
        spots = lax.broadcasted_iota(jnp.int32, (1, t_rows), 1).astype(F32)
        oh[...] = (own == spots).astype(F32)
        for t in range(n):
            held = (picks >= t * t_rows) & (picks < (t + 1) * t_rows)
            count = jnp.sum(held.astype(F32), axis=1, keepdims=True)
            counts[t] = jnp.broadcast_to(count, (1, HEAD_DIM))
        load_tok.wait()
        hot = oh[...].astype(BF16)
        chunk = 512
        square = jnp.zeros((MOST_OWN, 1), F32)
        for i in range(width // chunk):
            cols = slice(i * chunk, (i + 1) * chunk)
            rows = jnp.dot(hot, tok_v[:, cols], preferred_element_type=F32)
            square = square + jnp.sum(rows * rows, axis=1, keepdims=True)
            normed[:, cols] = rows.astype(BF16)
        scale = lax.rsqrt(square / width + 1e-06)
        for i in range(width // chunk):
            cols = slice(i * chunk, (i + 1) * chunk)
            normed[:, cols] = (normed[:, cols].astype(F32) * scale).astype(BF16)

    def place_gates(i):
        tile = t_rows // TILES
        low = i * tile
        oh_out[low : low + tile, :] = oh[:, low : low + tile].T.astype(BF16)
        spot = lax.broadcasted_iota(jnp.int32, (tile, 1), 0) + (seq * t_rows + low)
        gate = jnp.sum(jnp.where(ch[...] == spot, gates[...], 0.0), axis=1, keepdims=True)
        gate_out[low : low + tile, :] = jnp.broadcast_to(gate, (tile, HEAD_DIM))

    def project_kv():
        for e in range(KV_HEADS):
            part = jnp.dot(
                normed[...], kvw[:, e * pair : (e + 1) * pair], preferred_element_type=F32
            )
            kv[seq, e, 0] = part[:, :HEAD_DIM].astype(BF16)
            flip = part[:, HEAD_DIM:].T.astype(BF16)
            kv[seq, e, 1, :HEAD_DIM, :] = flip[:, :HEAD_DIM]
            kv[seq, e, 1, HEAD_DIM:, :] = flip[:, HEAD_DIM:]

    def project_q():
        for i in range(HEADS // 2):
            part = jnp.dot(
                normed[...], qw[:, i * pair : (i + 1) * pair], preferred_element_type=F32
            )
            part = part * HEAD_DIM**-0.5
            for h in range(2):
                head = i * 2 + h
                e, first = head // group, (head % group) * MOST_OWN
                flip = part[:, h * HEAD_DIM : (h + 1) * HEAD_DIM].T.astype(BF16)
                qt[e, :HEAD_DIM, first : first + MOST_OWN] = flip
        row = lax.broadcasted_iota(jnp.int32, (HEAD_DIM, group * MOST_OWN), 0)
        for e in range(KV_HEADS):
            qt[e, HEAD_DIM:, :] = (row == 0).astype(F32).astype(BF16)

    def attend(t, diagonal):
        row = lax.broadcasted_iota(jnp.int32, (MOST_OWN, HEAD_DIM), 0).astype(F32)
        bias = jnp.where(row < counts[t], 0.0, NEG).astype(BF16)
        ones = jnp.ones((ONES, MOST_OWN), BF16)
        heads = range(HEADS)
        left, right = [], []
        for e in range(KV_HEADS):
            left.append(jnp.concatenate([kv[t, e, 0], bias], axis=1))
            flip = [kv[t, e, 1, :HEAD_DIM, :], kv[t, e, 1, HEAD_DIM:, :]]
            right.append(jnp.concatenate([jnp.concatenate(flip, axis=1), ones], axis=0))
        score = []
        for f in heads:
            first = (f % group) * MOST_OWN
            query = qt[f // group, :, first : first + MOST_OWN]
            score.append(jnp.dot(left[f // group], query, preferred_element_type=F32))
        if diagonal:
            key = lax.broadcasted_iota(jnp.int32, (MOST_OWN, MOST_OWN), 0)
            asks = lax.broadcasted_iota(jnp.int32, (MOST_OWN, MOST_OWN), 1)
            score = [jnp.where(key <= asks, s, NEG) for s in score]
            top = [jnp.max(s, axis=0, keepdims=True) for s in score]
        else:
            old = [m_s[f] for f in heads]
            held = [acc[f] for f in heads]
            top = [
                jnp.maximum(o, jnp.max(s, axis=0, keepdims=True)) for o, s in zip(old, score)
            ]
        prob = [jnp.exp(s - m).astype(BF16) for s, m in zip(score, top)]
        new = [
            jnp.dot(right[f // group], prob[f], preferred_element_type=F32) for f in heads
        ]
        if not diagonal:
            new = [h * jnp.exp(o - m) + v for h, o, m, v in zip(held, old, top, new)]
        for f in heads:
            m_s[f] = top[f]
            acc[f] = new[f]

    def attend_past(k, j):
        pl.when(K.has(k, j))(lambda: attend(piece_of(geo, k, j), False))

    def finish_attention():
        for f in range(HEADS):
            total = acc[f]
            flip = (total[:HEAD_DIM] / total[HEAD_DIM : HEAD_DIM + 1]).T
            att[:, f * HEAD_DIM : (f + 1) * HEAD_DIM] = flip.astype(BF16)

    def project_out(k, j):
        if o_cols % 128 == 0:
            s = piece_of(geo, k, j)
            cols = pl.ds(pl.multiple_of(s * o_cols, o_cols), o_cols)
            blk[:, cols] = jnp.dot(
                att[...], obuf[s], preferred_element_type=F32
            ).astype(BF16)

    tasks = {
        "gather": gather,
        "gates": place_gates,
        "kv": project_kv,
        "q": project_q,
        "own": lambda: attend(seq, True),
        "att": attend_past,
        "norm": finish_attention,
        "out": project_out,
    }
    for what, *at in plan_of(A, B):
        if what in tasks:
            tasks[what](*at)
            continue
        if what == "K":
            kind, k, j, e = at
            if kind == "z":
                K.slow(k, e)
            else:
                K.fast(k, j, e)
            continue
        ring = rings[what]
        kind, k, j = at
        if kind in ("oz", "ox"):
            for made in loads[what]:
                made.wait()
            loads[what] = []
        if kind == "oz":
            ring.send_z(0)
        elif kind == "ox":
            ring.send_x(0)
        elif kind == "z":
            ring.slow(k)
        elif kind == "x":
            ring.fast(k, j)
        elif kind == "ys":
            ring.send_y(k, j)
        elif kind == "y":
            ring.relay(k, j)
        else:
            ring.from_core(k, j)
    if o_cols % 128 != 0:
        for s in range(n):
            blk[:, s * o_cols : (s + 1) * o_cols] = jnp.dot(
                att[...], obuf[s], preferred_element_type=F32
            ).astype(BF16)
    for ring in (W, Q, O, K):
        ring.finish()


def add_kernel(tok, gate, oh, blk, out, made, sems):
    tile = tok.shape[0] // ADD_TILES
    copies = []
    for i in range(ADD_TILES):
        rows = pl.ds(i * tile, tile)
        for first in range(0, tok.shape[1], 2 * HEAD_DIM):
            right = blk[:, first : first + 2 * HEAD_DIM]
            lift = jnp.dot(oh[rows, :], right, preferred_element_type=F32)
            for j in range(0, 2 * HEAD_DIM, HEAD_DIM):
                cols = slice(first + j, first + j + HEAD_DIM)
                added = gate[rows, :] * lift[:, j : j + HEAD_DIM]
                made[rows, cols] = (tok[rows, cols].astype(F32) + added).astype(BF16)
        copies.append(pltpu.make_async_copy(made.at[rows], out.at[rows], sems.at[i]))
        copies[-1].start()
    for copy in copies:
        copy.wait()


def in_hbm(array):
    return pltpu.with_memory_space_constraint(array, pltpu.HBM)


def per_device(tokens, chosen, gates, w_query, w_key, w_value, w_out):
    n = lax.axis_size("seq")
    A = 4 if n % 4 == 0 else 1
    B = n // A
    t_rows, width = tokens.shape
    k_rows, q_cols = w_query.shape
    e_cols = w_key.shape[1]
    o_rows, o_cols = w_out.shape
    picks = chosen.reshape(1, -1)
    gate_row = gates.reshape(1, -1)
    dma = pltpu.SemaphoreType.DMA
    hbm_spec = pl.BlockSpec(memory_space=pltpu.HBM)
    vmem_spec = pl.BlockSpec(memory_space=pltpu.VMEM)
    steps_x = max(A * (B - 1), 1)
    steps_z = max(A - 1, 1)

    def pair(count):
        return (dma((count,)), dma((count,)))

    sems = []
    for _ in range(3):
        sems += [pair(steps_z), pair(steps_x), pair(n - 1), pair(2 * (n - 1))]
    sems += [pair(KV_HEADS * steps_z), pair(KV_HEADS * steps_x), pair(KV_HEADS)]
    flat = [x for two in sems for x in two]

    def body(*refs):
        head, tail = refs[: len(refs) - len(flat)], refs[len(refs) - len(flat) :]
        pairs = [(tail[i], tail[i + 1]) for i in range(0, len(tail), 2)]
        main_kernel(A, B, *head, *pairs)

    blk, oh, gate = pl.pallas_call(
        body,
        out_shape=(
            jax.ShapeDtypeStruct((MOST_OWN, width), BF16),
            jax.ShapeDtypeStruct((t_rows, MOST_OWN), BF16),
            jax.ShapeDtypeStruct((t_rows, HEAD_DIM), F32),
        ),
        in_specs=[hbm_spec] * 7,
        out_specs=(vmem_spec, vmem_spec, vmem_spec),
        scratch_shapes=[
            pltpu.VMEM(picks.shape, jnp.int32),
            pltpu.VMEM(picks.shape, F32),
            pltpu.VMEM((MOST_OWN, t_rows), F32),
            pltpu.VMEM((t_rows, width), BF16),
            pltpu.VMEM((n * k_rows, 2 * e_cols), BF16),
            pltpu.VMEM((n * k_rows, q_cols), BF16),
            pltpu.VMEM((n, o_rows, o_cols), BF16),
            pltpu.VMEM((n, KV_HEADS, 2, MOST_OWN, HEAD_DIM), BF16),
            pltpu.VMEM((MOST_OWN, width), BF16),
            pltpu.VMEM((KV_HEADS, 2 * HEAD_DIM, HEADS // KV_HEADS * MOST_OWN), BF16),
            pltpu.VMEM((HEADS, HEAD_DIM + ONES, MOST_OWN), F32),
            pltpu.VMEM((HEADS, 1, MOST_OWN), F32),
            pltpu.VMEM((n, 1, HEAD_DIM), F32),
            pltpu.VMEM((MOST_OWN, HEADS * HEAD_DIM), BF16),
            dma((2 * KV_HEADS + 5,)),
            *flat,
        ],
        compiler_params=pltpu.CompilerParams(
            collective_id=0, has_side_effects=True, vmem_limit_bytes=MAIN_VMEM * 1024 * 1024
        ),
        name="gather_attend",
    )(
        *map(in_hbm, (tokens, picks, gate_row, w_query, w_key, w_value, w_out))
    )

    return pl.pallas_call(
        add_kernel,
        out_shape=jax.ShapeDtypeStruct((t_rows, width), BF16),
        in_specs=[vmem_spec] * 4,
        out_specs=hbm_spec,
        scratch_shapes=[pltpu.VMEM((t_rows, width), BF16), dma((ADD_TILES,))],
        compiler_params=pltpu.CompilerParams(vmem_limit_bytes=ADD_VMEM * 1024 * 1024),
        name="add_rows",
    )(tokens, gate, oh, blk)


def solution(mesh):
    return jax.shard_map(
        per_device,
        mesh=mesh,
        in_specs=(
            P(("dp", "seq"), None),
            P("dp"),
            P("dp"),
            P("seq", None),
            P("seq", None),
            P("seq", None),
            P(None, "seq"),
        ),
        out_specs=P(("dp", "seq"), None),
        check_vma=False,
    )
```

```python
import functools

import jax
import jax.numpy as jnp
from jax import lax
from jax.experimental import pallas as pl
from jax.experimental.pallas import tpu as pltpu
from jax.sharding import PartitionSpec as P

HEADS = 8
KV_HEADS = 2
HEAD_DIM = 128
MOST_OWN = 256
ONES = 16
TILES = 4
ADD_TILES = 4
MAIN_VMEM = 36
ADD_VMEM = 12
Q_SHARE = 9
O_SHARE = 18
PLAN = (
    ("W", "oz", 0, 0), ("W", "ox", 0, 0), ("Q", "ox", 0, 0), ("Q", "oz", 0, 0), ("gather",),
    ("W", "x", 0, 1), ("W", "ys", 0, 1), ("W", "z", 1, 0), ("W", "xe", 0, 0), ("W", "ys", 1, 0),
    ("W", "z", 2, 0), ("O", "ox", 0, 0), ("W", "ys", 2, 0), ("O", "oz", 0, 0), ("Q", "x", 0, 1),
    ("Q", "ys", 0, 1), ("W", "x", 1, 1), ("W", "ys", 1, 1), ("W", "z", 3, 0), ("gates", 0),
    ("W", "ys", 3, 0), ("W", "y", 1, 0), ("gates", 2), ("Q", "z", 1, 0), ("W", "y", 2, 0),
    ("W", "x", 2, 1), ("Q", "ys", 1, 0), ("W", "y", 0, 1), ("W", "ys", 2, 1), ("Q", "z", 2, 0),
    ("W", "y", 1, 1), ("W", "e", 2, 0), ("W", "x", 3, 1), ("O", "z", 1, 0), ("W", "ys", 3, 1),
    ("O", "z", 2, 0), ("O", "ys", 2, 0), ("Q", "x", 1, 1), ("Q", "ys", 2, 0), ("W", "y", 3, 0),
    ("Q", "z", 3, 0), ("W", "e", 1, 1), ("W", "e", 1, 0), ("W", "e", 3, 0), ("Q", "ys", 1, 1),
    ("W", "y", 2, 1), ("Q", "x", 2, 1), ("Q", "xe", 0, 0), ("W", "y", 3, 1), ("W", "e", 2, 1),
    ("O", "z", 3, 0), ("Q", "y", 1, 0), ("W", "e", 3, 1), ("W", "e", 0, 1), ("kv",),
    ("Q", "ys", 2, 1), ("K", "z", 0, 0, 1), ("O", "ys", 1, 0), ("K", "z", 0, 0, 0),
    ("Q", "ys", 3, 0), ("O", "x", 0, 1), ("O", "y", 2, 0), ("Q", "y", 1, 1), ("O", "e", 2, 0),
    ("Q", "x", 3, 1), ("Q", "y", 2, 0), ("Q", "ys", 3, 1), ("O", "x", 2, 1), ("O", "x", 1, 1),
    ("K", "z", 1, 0, 1), ("Q", "e", 1, 1), ("gates", 1), ("K", "z", 1, 0, 0), ("O", "ys", 2, 1),
    ("Q", "e", 2, 0), ("O", "ys", 3, 0), ("Q", "y", 3, 0), ("Q", "e", 1, 0), ("O", "ys", 0, 1),
    ("Q", "y", 0, 1), ("O", "y", 1, 0), ("O", "ys", 1, 1), ("K", "x", 0, 1, 1), ("K", "z", 2, 0, 1),
    ("Q", "e", 3, 0), ("O", "xe", 0, 0), ("O", "x", 3, 1), ("Q", "e", 0, 1), ("gates", 3),
    ("O", "e", 1, 0), ("O", "ys", 3, 1), ("Q", "y", 2, 1), ("Q", "y", 3, 1), ("K", "z", 2, 0, 0),
    ("Q", "e", 3, 1), ("Q", "e", 2, 1), ("K", "x", 0, 1, 0), ("q",), ("own",), ("O", "y", 2, 1),
    ("K", "z", 3, 0, 1), ("att", 0, 1), ("att", 2, 0), ("K", "x", 1, 1, 1), ("K", "z", 3, 0, 0),
    ("O", "y", 0, 1), ("O", "y", 3, 0), ("att", 3, 0), ("att", 1, 0), ("K", "x", 1, 1, 0),
    ("O", "y", 1, 1), ("O", "e", 2, 1), ("O", "e", 0, 1), ("O", "e", 3, 0), ("K", "x", 3, 1, 1),
    ("K", "x", 2, 1, 1), ("att", 1, 1), ("K", "x", 2, 1, 0), ("O", "e", 1, 1), ("att", 2, 1),
    ("O", "y", 3, 1), ("K", "x", 3, 1, 0), ("att", 3, 1), ("norm",), ("out", 0, 0), ("out", 3, 0),
    ("out", 0, 1), ("out", 2, 1), ("O", "e", 3, 1), ("out", 1, 0), ("out", 3, 1), ("out", 2, 0),
    ("out", 1, 1),
)
MESH = pl.DeviceIdType.MESH
NEG = -1e30
F32 = jnp.float32
BF16 = jnp.bfloat16


class Ring:
    def __init__(self, geo, sems, region_in, region_y):
        self.g = geo
        self.sems = sems
        self.region_in = region_in
        self.region_y = region_y
        self.sends = []
        self.some = []
        self.whole = geo["B"] == 2
        a_count, b_count = geo["A"], geo["B"]
        self.order = arrivals(a_count, b_count)

    def piece(self, k, j):
        g = self.g
        b = lax.rem(g["b"] - j + g["B"], g["B"])
        return at_row(g, lambda row: by_distance(g["A"], row)[k]) * g["B"] + b

    def copy(self, kind, index, ref, dp, seq):
        return remote(ref, self.sems["sent"].at[0], self.sems[kind].at[index], dp, seq)

    def send(self, *args):
        made = self.copy(*args)
        made.start()
        self.sends.append(made)

    def arrive(self, kind, index, ref):
        self.copy(kind, index, ref, self.g["dp"], self.g["x_next"]).wait_recv()

    def mine(self, s):
        return self.region_in(s, self.g["y"], self.g["c"])

    def send_core(self, k, j):
        g = self.g
        self.send("d", self.order.index((k, j)), self.mine(self.piece(k, j)), g["dp_c"], g["seq"])

    def send_y(self, k, j):
        g = self.g
        ref = self.region_y(self.piece(k, j), g["y"], g["c"])
        args = ("y", self.order.index((k, j)), ref, g["dp_y"], g["seq"])
        if self.whole and (k, j) == (0, 1):
            self.send_if(g["a"] > 0, *args)
        else:
            self.send(*args)

    def send_rest(self):
        g = self.g
        if self.whole:
            ref = self.region_y(self.piece(0, 0), 1 - g["y"], g["c"])
            self.send_if(g["a"] == 0, "r", 0, ref, g["dp"], g["x_next"])

    def send_if(self, cond, *args):
        made = self.copy(*args)
        pl.when(cond)(made.start)
        self.some.append((cond, made))

    def send_z(self):
        g = self.g
        mine = self.mine(self.piece(0, 0))
        self.send_if(g["a"] < g["A"] - 1, "u", 0, mine, g["dp"], g["z_up"])
        self.send_if(g["a"] > 0, "v", 0, mine, g["dp"], g["z_down"])

    def take_z(self, k):
        g = self.g
        mine = self.mine(self.piece(k, 0))
        for far in range(1, g["A"]):
            for kind, sign, to in (("u", -1, g["z_up"]), ("v", 1, g["z_down"])):
                rows = [
                    row
                    for row in range(g["A"])
                    if by_distance(g["A"], row)[k] == row + sign * far
                ]
                if not rows:
                    continue
                here = any_row(g, rows)
                pl.when(here)(self.copy(kind, far - 1, mine, g["dp"], to).wait_recv)
                onward = [row for row in rows if 0 <= row - sign < g["A"]]
                if onward:
                    self.send_if(any_row(g, onward), kind, far, mine, g["dp"], to)

    def send_x(self, k):
        g = self.g
        if g["B"] > 1:
            ref = self.mine(self.piece(k, 0))
            self.send("x", k * (g["B"] - 1), ref, g["dp"], g["x_next"])

    def slow(self, k):
        self.take_z(k)
        self.send_x(k)
        self.send_core(k, 0)

    def fast(self, k, j):
        g = self.g
        s = self.piece(k, j)
        self.arrive("x", k * (g["B"] - 1) + j - 1, self.mine(s))
        if j < g["B"] - 1:
            self.send("x", k * (g["B"] - 1) + j, self.mine(s), g["dp"], g["x_next"])
        self.send_core(k, j)

    def relay(self, k, j):
        g = self.g
        index = self.order.index((k, j))
        ref = self.region_y(self.piece(k, j), 1 - g["y"], g["c"])
        if self.whole and (k, j) == (0, 1):
            rest = self.copy("r", 0, ref, g["dp"], g["x_next"])
            over = self.copy("y", index, ref, g["dp_y"], g["seq"])
            pl.when(g["a"] == 0)(rest.wait_recv)
            pl.when(g["a"] > 0)(over.wait_recv)
        else:
            self.arrive("y", index, ref)
        self.send("d", len(self.order) + index, ref, g["dp_c"], g["seq"])

    def from_core(self, k, j):
        g = self.g
        index = self.order.index((k, j))
        s = self.piece(k, j)
        self.arrive("d", index, self.region_in(s, g["y"], 1 - g["c"]))
        self.arrive("d", len(self.order) + index, self.region_y(s, 1 - g["y"], 1 - g["c"]))

    def finish(self):
        for made in self.sends:
            made.wait_send()
        for cond, made in self.some:
            pl.when(cond)(made.wait_send)


class Causal:
    def __init__(self, geo, sems, ref, parts):
        self.g = geo
        self.sems = sems
        self.ref = ref
        self.parts = parts
        self.sends = []
        self.detour = geo["B"] == 2 and geo["A"] >= 2
        self.last = geo["a"] == geo["A"] - 1

    def has(self, k, j):
        g = self.g
        if k > 0:
            return g["a"] >= k
        return g["b"] >= j

    def copy(self, kind, index, e, s, seq):
        recv = self.sems[kind].at[index * self.parts + e]
        return remote(self.ref(s, e), self.sems["sent"].at[0], recv, self.g["dp"], seq)

    def send(self, cond, *args):
        made = self.copy(*args)
        pl.when(cond)(made.start)
        self.sends.append((cond, made))

    def arrive(self, cond, *args):
        pl.when(cond)(self.copy(*args, self.g["z_up"]).wait_recv)

    def slow(self, k, e):
        g = self.g
        s = piece_of(g, k, 0)
        if k > 0:
            self.arrive(g["a"] >= k, "z", k - 1, e, s)
        if k < g["A"] - 1:
            cond = jnp.logical_and(g["a"] >= k, g["a"] + 1 < g["A"])
            self.send(cond, "z", k, e, s, g["z_up"])
        if g["B"] > 1:
            cond = g["a"] >= k if k > 0 else g["b"] + 1 < g["B"]
            if self.detour and k == 1:
                turned = jnp.logical_and(self.last, g["b"] == 0)
                cond = jnp.logical_and(cond, jnp.logical_not(turned))
            self.send(cond, "x", k * (g["B"] - 1), e, s, g["x_next"])

    def fast(self, k, j, e):
        g = self.g
        s = piece_of(g, k, j)
        index = k * (g["B"] - 1) + j - 1
        has = self.has(k, j)
        if self.detour and k == 1:
            turned = jnp.logical_and(self.last, g["b"] == 1)
            self.arrive(turned, "t", 0, e, s)
            has = jnp.logical_and(has, jnp.logical_not(turned))
        self.arrive(has, "x", index, e, s)
        if self.detour and k == 0:
            cond = jnp.logical_and(g["a"] == g["A"] - 2, g["b"] == 1)
            self.send(cond, "t", 0, e, s, g["z_up"])
        if j < g["B"] - 1:
            cond = self.has(k, j)
            if k == 0:
                cond = jnp.logical_and(cond, g["b"] + 1 < g["B"])
            self.send(cond, "x", index + 1, e, s, g["x_next"])

    def finish(self):
        for cond, made in self.sends:
            pl.when(cond)(made.wait_send)


def remote(ref, send, recv, dp, seq):
    return pltpu.make_async_remote_copy(
        src_ref=ref,
        dst_ref=ref,
        send_sem=send,
        recv_sem=recv,
        device_id=(dp, seq),
        device_id_type=MESH,
    )


def arrivals(a_count, b_count):
    order = []
    for k in range(1, a_count):
        order += [(k, 0)] + [(k - 1, j) for j in range(1, b_count)]
    return order + [(a_count - 1, j) for j in range(1, b_count)]


def by_distance(count, row):
    return sorted(range(count), key=lambda other: (abs(other - row), other))


def at_row(g, value):
    result = value(0)
    for row in range(1, g["A"]):
        result = jnp.where(g["a"] == row, value(row), result)
    return result


def any_row(g, rows):
    result = g["a"] == rows[0]
    for row in rows[1:]:
        result = jnp.logical_or(result, g["a"] == row)
    return result


def piece_of(g, k, j):
    a = lax.rem(g["a"] - k + g["A"], g["A"])
    b = lax.rem(g["b"] - j + g["B"], g["B"])
    return a * g["B"] + b


def plan_of(A, B):
    if (A, B) == (4, 2):
        return PLAN
    order = arrivals(A, B)
    taken = {kj: ("z" if kj[1] == 0 else "x", *kj) for kj in order}
    parts = range(KV_HEADS)
    plan = [("gather",)]
    for what in "WQ":
        plan += [(what, "oz", 0, 0), (what, "ox", 0, 0)]
    for what in "WQ":
        for kj in order:
            plan += [(what, *taken[kj]), (what, "ys", *kj)]
    for what in "O":
        plan += [(what, "oz", 0, 0), (what, "ox", 0, 0)]
    plan += [("W", "y", *kj) for kj in order] + [("W", "e", *kj) for kj in order]
    plan += [("gates", i) for i in range(TILES)] + [("kv",)]
    plan += [("K", "z", 0, 0, e) for e in parts]
    for kj in order[: len(order) // 2]:
        for what in "O":
            plan += [(what, *taken[kj]), (what, "ys", *kj)]
    for what in "Q":
        plan += [(what, "y", *kj) for kj in order] + [(what, "e", *kj) for kj in order]
    plan += [("q",), ("own",)]
    for i, kj in enumerate(order):
        plan += [("K", *taken[kj], e) for e in parts] + [("att", *kj)]
        if i >= len(order) // 2:
            for what in "O":
                plan += [(what, *taken[kj]), (what, "ys", *kj)]
    for what in "O":
        plan += [(what, "y", *kj) for kj in order]
    plan += [("norm",), ("out", 0, 0)]
    for kj in order:
        plan += [(what, "e", *kj) for what in "O"] + [("out", *kj)]
    return plan


def up16(value):
    return (value + 15) // 16 * 16


def main_kernel(
    A, B, tok, ch_in, gates_in, wq, wk, wv, wo, blk, oh_out, gate_out,
    ch, gates, oh, tok_v, kvw, qw, obuf, kv, normed, qt, acc, m_s, counts, att, lsem,
    sent, *sems,
):
    n = A * B
    dp = lax.axis_index("dp")
    seq = lax.axis_index("seq")
    a, b = seq // B, lax.rem(seq, B)
    y, c = lax.rem(dp // 2, 2), lax.rem(dp, 2)
    z_up = lax.rem(a + 1, A) * B + b
    z_down = lax.rem(a + A - 1, A) * B + b
    x_next = a * B + lax.rem(b + 1, B)
    x_prev = a * B + lax.rem(b + B - 1, B)
    dp_y = dp + 2 * (1 - 2 * y)
    dp_c = dp + 1 - 2 * c
    geo = dict(
        A=A, B=B, a=a, b=b, y=y, c=c, dp=dp, seq=seq,
        z_up=z_up, z_down=z_down, x_next=x_next, dp_y=dp_y, dp_c=dp_c,
    )
    t_rows = tok.shape[0]
    width = tok.shape[1]
    k_rows = wq.shape[0]
    q_cols, e_cols = wq.shape[1], wk.shape[1]
    o_rows, o_cols = wo.shape
    group = HEADS // KV_HEADS
    pair = 2 * HEAD_DIM

    rows_here = pl.ds(pl.multiple_of(seq * k_rows, k_rows), k_rows)
    local = []
    for e in range(KV_HEADS):
        cols = pl.ds(e * HEAD_DIM, HEAD_DIM)
        local.append((wk.at[:, cols], kvw.at[rows_here, pl.ds(e * pair, HEAD_DIM)]))
        local.append((wv.at[:, cols], kvw.at[rows_here, pl.ds(e * pair + HEAD_DIM, HEAD_DIM)]))
    local += [(wq, qw.at[rows_here, :]), (ch_in, ch), (tok, tok_v), (wo, obuf.at[seq])]
    local += [(gates_in, gates)]
    local = [pltpu.make_async_copy(s, d, lsem.at[i]) for i, (s, d) in enumerate(local)]
    for made in local:
        made.start()
    load_kv, rest = local[: 2 * KV_HEADS], local[2 * KV_HEADS :]
    load_q, load_ch, load_tok, load_o, load_gates = rest

    greet = [(dp_y, seq), (dp_c, seq)]
    if B > 1:
        greet += [(dp, x_next)] + ([(dp, x_prev)] if B > 2 else [])
    barrier = pltpu.get_barrier_semaphore()

    def hail(who):
        pl.semaphore_signal(barrier, inc=1, device_id=who, device_id_type=MESH)

    for who in greet:
        hail(who)
    if A > 1:
        inner = jnp.logical_and(a > 0, a < A - 1)
        pl.when(a < A - 1)(lambda: hail((dp, z_up)))
        pl.when(a > 0)(lambda: hail((dp, z_down)))
        pl.when(inner)(lambda: pl.semaphore_wait(barrier, len(greet) + 2))
        pl.when(jnp.logical_not(inner))(lambda: pl.semaphore_wait(barrier, len(greet) + 1))
    else:
        pl.semaphore_wait(barrier, len(greet))

    quarter = 2 * e_cols // 4

    def w_region(s, y, c):
        return kvw.at[
            pl.ds(pl.multiple_of(s * k_rows, k_rows), k_rows),
            pl.ds(pl.multiple_of((2 * c + y) * quarter, 128), quarter),
        ]

    q_half = q_cols // 2
    q_in = up16(k_rows * Q_SHARE // 16)

    def q_region(s, c, start, size):
        return qw.at[
            pl.ds(pl.multiple_of(s * k_rows + start, 16), size),
            pl.ds(pl.multiple_of(c * q_half, 128), q_half),
        ]

    o_half = o_rows // 2
    o_in = up16(o_half * O_SHARE // 32)

    def o_region(s, start, size):
        return obuf.at[s, pl.ds(pl.multiple_of(start, 16), size), :]

    w_sems, q_sems, o_sems = (
        dict(zip("uvxydr", sems[6 * i : 6 * i + 6]), sent=sent) for i in range(3)
    )
    kz, kx, kt = sems[18:]
    W = Ring(geo, w_sems, w_region, w_region)
    Q = Ring(
        geo,
        q_sems,
        lambda s, y, c: q_region(s, c, y * (k_rows - q_in), q_in),
        lambda s, y, c: q_region(s, c, y * q_in, k_rows - q_in),
    )
    O = Ring(
        geo,
        o_sems,
        lambda s, y, c: o_region(s, c * o_half + y * (o_half - o_in), o_in),
        lambda s, y, c: o_region(s, c * o_half + y * o_in, o_half - o_in),
    )
    rings = {"W": W, "Q": Q, "O": O}
    loads = {"W": load_kv, "Q": [load_q], "O": [load_o]}
    K = Causal(geo, {"z": kz, "x": kx, "t": kt, "sent": sent}, lambda s, e: kv.at[s, e], KV_HEADS)

    def gather():
        load_ch.wait()
        load_gates.wait()
        base = seq * t_rows
        picks = ch[...]
        start = jnp.sum((picks < base).astype(F32), axis=1, keepdims=True)
        rel = picks - base
        inside = (rel >= 0) & (rel < t_rows)
        place = jnp.where(inside, (rel + 1).astype(F32), 0.0)
        rank = lax.broadcasted_iota(jnp.int32, picks.shape, 1).astype(F32) - start
        slots = lax.broadcasted_iota(jnp.int32, (MOST_OWN, 1), 0).astype(F32)
        own = jnp.sum(jnp.where(rank == slots, place, 0.0), axis=1, keepdims=True) - 1.0
        spots = lax.broadcasted_iota(jnp.int32, (1, t_rows), 1).astype(F32)
        oh[...] = (own == spots).astype(F32)
        for t in range(n):
            held = (picks >= t * t_rows) & (picks < (t + 1) * t_rows)
            count = jnp.sum(held.astype(F32), axis=1, keepdims=True)
            counts[t] = jnp.broadcast_to(count, (1, HEAD_DIM))
        load_tok.wait()
        hot = oh[...].astype(BF16)
        chunk = 512
        square = jnp.zeros((MOST_OWN, 1), F32)
        for i in range(width // chunk):
            cols = slice(i * chunk, (i + 1) * chunk)
            rows = jnp.dot(hot, tok_v[:, cols], preferred_element_type=F32)
            square = square + jnp.sum(rows * rows, axis=1, keepdims=True)
            normed[:, cols] = rows.astype(BF16)
        scale = lax.rsqrt(square / width + 1e-06)
        for i in range(width // chunk):
            cols = slice(i * chunk, (i + 1) * chunk)
            normed[:, cols] = (normed[:, cols].astype(F32) * scale).astype(BF16)

    def place_gates(i):
        tile = t_rows // TILES
        low = i * tile
        oh_out[low : low + tile, :] = oh[:, low : low + tile].T.astype(BF16)
        spot = lax.broadcasted_iota(jnp.int32, (tile, 1), 0) + (seq * t_rows + low)
        gate = jnp.sum(jnp.where(ch[...] == spot, gates[...], 0.0), axis=1, keepdims=True)
        gate_out[low : low + tile, :] = jnp.broadcast_to(gate, (tile, HEAD_DIM))

    def project_kv():
        for e in range(KV_HEADS):
            part = jnp.dot(
                normed[...], kvw[:, e * pair : (e + 1) * pair], preferred_element_type=F32
            )
            kv[seq, e, 0] = part[:, :HEAD_DIM].astype(BF16)
            flip = part[:, HEAD_DIM:].T.astype(BF16)
            kv[seq, e, 1, :HEAD_DIM, :] = flip[:, :HEAD_DIM]
            kv[seq, e, 1, HEAD_DIM:, :] = flip[:, HEAD_DIM:]

    def project_q():
        for i in range(HEADS // 2):
            part = jnp.dot(
                normed[...], qw[:, i * pair : (i + 1) * pair], preferred_element_type=F32
            )
            part = part * HEAD_DIM**-0.5
            for h in range(2):
                head = i * 2 + h
                e, first = head // group, (head % group) * MOST_OWN
                flip = part[:, h * HEAD_DIM : (h + 1) * HEAD_DIM].T.astype(BF16)
                qt[e, :HEAD_DIM, first : first + MOST_OWN] = flip
        row = lax.broadcasted_iota(jnp.int32, (HEAD_DIM, group * MOST_OWN), 0)
        for e in range(KV_HEADS):
            qt[e, HEAD_DIM:, :] = (row == 0).astype(F32).astype(BF16)

    def attend(t, diagonal):
        row = lax.broadcasted_iota(jnp.int32, (MOST_OWN, HEAD_DIM), 0).astype(F32)
        bias = jnp.where(row < counts[t], 0.0, NEG).astype(BF16)
        ones = jnp.ones((ONES, MOST_OWN), BF16)
        heads = range(HEADS)
        left, right = [], []
        for e in range(KV_HEADS):
            left.append(jnp.concatenate([kv[t, e, 0], bias], axis=1))
            flip = [kv[t, e, 1, :HEAD_DIM, :], kv[t, e, 1, HEAD_DIM:, :]]
            right.append(jnp.concatenate([jnp.concatenate(flip, axis=1), ones], axis=0))
        score = []
        for f in heads:
            first = (f % group) * MOST_OWN
            query = qt[f // group, :, first : first + MOST_OWN]
            score.append(jnp.dot(left[f // group], query, preferred_element_type=F32))
        if diagonal:
            key = lax.broadcasted_iota(jnp.int32, (MOST_OWN, MOST_OWN), 0)
            asks = lax.broadcasted_iota(jnp.int32, (MOST_OWN, MOST_OWN), 1)
            score = [jnp.where(key <= asks, s, NEG) for s in score]
            top = [jnp.max(s, axis=0, keepdims=True) for s in score]
        else:
            old = [m_s[f] for f in heads]
            held = [acc[f] for f in heads]
            top = [
                jnp.maximum(o, jnp.max(s, axis=0, keepdims=True)) for o, s in zip(old, score)
            ]
        prob = [jnp.exp(s - m).astype(BF16) for s, m in zip(score, top)]
        new = [
            jnp.dot(right[f // group], prob[f], preferred_element_type=F32) for f in heads
        ]
        if not diagonal:
            new = [h * jnp.exp(o - m) + v for h, o, m, v in zip(held, old, top, new)]
        for f in heads:
            m_s[f] = top[f]
            acc[f] = new[f]

    def attend_past(k, j):
        pl.when(K.has(k, j))(lambda: attend(piece_of(geo, k, j), False))

    def finish_attention():
        for f in range(HEADS):
            total = acc[f]
            flip = (total[:HEAD_DIM] / total[HEAD_DIM : HEAD_DIM + 1]).T
            att[:, f * HEAD_DIM : (f + 1) * HEAD_DIM] = flip.astype(BF16)

    def project_out(k, j):
        if o_cols % 128 == 0:
            s = W.piece(k, j)
            cols = pl.ds(pl.multiple_of(s * o_cols, o_cols), o_cols)
            blk[:, cols] = jnp.dot(
                att[...], obuf[s], preferred_element_type=F32
            ).astype(BF16)

    tasks = {
        "gather": gather,
        "gates": place_gates,
        "kv": project_kv,
        "q": project_q,
        "own": lambda: attend(seq, True),
        "att": attend_past,
        "norm": finish_attention,
        "out": project_out,
    }
    for what, *at in plan_of(A, B):
        if what in tasks:
            tasks[what](*at)
            continue
        if what == "K":
            kind, k, j, e = at
            if kind == "z":
                K.slow(k, e)
            else:
                K.fast(k, j, e)
            continue
        ring = rings[what]
        kind, k, j = at
        if kind in ("oz", "ox", "xe"):
            for made in loads[what]:
                made.wait()
            loads[what] = []
        if kind == "oz":
            ring.send_z()
        elif kind == "ox":
            ring.send_x(0)
        elif kind == "xe":
            ring.send_rest()
        elif kind == "z":
            ring.slow(k)
        elif kind == "x":
            ring.fast(k, j)
        elif kind == "ys":
            ring.send_y(k, j)
        elif kind == "y":
            ring.relay(k, j)
        else:
            ring.from_core(k, j)
    if o_cols % 128 != 0:
        for s in range(n):
            blk[:, s * o_cols : (s + 1) * o_cols] = jnp.dot(
                att[...], obuf[s], preferred_element_type=F32
            ).astype(BF16)
    for ring in (*rings.values(), K):
        ring.finish()


def add_kernel(tok, gate, oh, blk, out, made, sems):
    tile = tok.shape[0] // ADD_TILES
    copies = []
    for i in range(ADD_TILES):
        rows = pl.ds(i * tile, tile)
        for first in range(0, tok.shape[1], 2 * HEAD_DIM):
            right = blk[:, first : first + 2 * HEAD_DIM]
            lift = jnp.dot(oh[rows, :], right, preferred_element_type=F32)
            for j in range(0, 2 * HEAD_DIM, HEAD_DIM):
                cols = slice(first + j, first + j + HEAD_DIM)
                added = gate[rows, :] * lift[:, j : j + HEAD_DIM]
                made[rows, cols] = (tok[rows, cols].astype(F32) + added).astype(BF16)
        copies.append(pltpu.make_async_copy(made.at[rows], out.at[rows], sems.at[i]))
        copies[-1].start()
    for copy in copies:
        copy.wait()


def in_hbm(array):
    return pltpu.with_memory_space_constraint(array, pltpu.HBM)


def per_device(tokens, chosen, gates, w_query, w_key, w_value, w_out):
    n = lax.axis_size("seq")
    A = 4 if n % 4 == 0 else 1
    B = n // A
    t_rows, width = tokens.shape
    k_rows, q_cols = w_query.shape
    e_cols = w_key.shape[1]
    o_rows, o_cols = w_out.shape
    picks = chosen.reshape(1, -1)
    gate_row = gates.reshape(1, -1)
    dma = pltpu.SemaphoreType.DMA
    hbm_spec = pl.BlockSpec(memory_space=pltpu.HBM)
    vmem_spec = pl.BlockSpec(memory_space=pltpu.VMEM)
    steps_x = max(A * (B - 1), 1)
    steps_z = max(A - 1, 1)

    counts = [steps_z, steps_z, steps_x, n - 1, 2 * (n - 1), 1] * 3
    counts += [KV_HEADS * steps_z, KV_HEADS * steps_x, KV_HEADS]
    flat = [dma((1,))] + [dma((count,)) for count in counts]

    def body(*refs):
        main_kernel(A, B, *refs)

    blk, oh, gate = pl.pallas_call(
        body,
        out_shape=(
            jax.ShapeDtypeStruct((MOST_OWN, width), BF16),
            jax.ShapeDtypeStruct((t_rows, MOST_OWN), BF16),
            jax.ShapeDtypeStruct((t_rows, HEAD_DIM), F32),
        ),
        in_specs=[hbm_spec] * 7,
        out_specs=(vmem_spec, vmem_spec, vmem_spec),
        scratch_shapes=[
            pltpu.VMEM(picks.shape, jnp.int32),
            pltpu.VMEM(picks.shape, F32),
            pltpu.VMEM((MOST_OWN, t_rows), F32),
            pltpu.VMEM((t_rows, width), BF16),
            pltpu.VMEM((n * k_rows, 2 * e_cols), BF16),
            pltpu.VMEM((n * k_rows, q_cols), BF16),
            pltpu.VMEM((n, o_rows, o_cols), BF16),
            pltpu.VMEM((n, KV_HEADS, 2, MOST_OWN, HEAD_DIM), BF16),
            pltpu.VMEM((MOST_OWN, width), BF16),
            pltpu.VMEM((KV_HEADS, 2 * HEAD_DIM, HEADS // KV_HEADS * MOST_OWN), BF16),
            pltpu.VMEM((HEADS, HEAD_DIM + ONES, MOST_OWN), F32),
            pltpu.VMEM((HEADS, 1, MOST_OWN), F32),
            pltpu.VMEM((n, 1, HEAD_DIM), F32),
            pltpu.VMEM((MOST_OWN, HEADS * HEAD_DIM), BF16),
            dma((2 * KV_HEADS + 5,)),
            *flat,
        ],
        compiler_params=pltpu.CompilerParams(
            collective_id=0, has_side_effects=True, vmem_limit_bytes=MAIN_VMEM * 1024 * 1024
        ),
        name="gather_attend",
    )(
        *map(in_hbm, (tokens, picks, gate_row, w_query, w_key, w_value, w_out))
    )

    return pl.pallas_call(
        add_kernel,
        out_shape=jax.ShapeDtypeStruct((t_rows, width), BF16),
        in_specs=[vmem_spec] * 4,
        out_specs=hbm_spec,
        scratch_shapes=[pltpu.VMEM((t_rows, width), BF16), dma((ADD_TILES,))],
        compiler_params=pltpu.CompilerParams(vmem_limit_bytes=ADD_VMEM * 1024 * 1024),
        name="add_rows",
    )(tokens, gate, oh, blk)


def solution(mesh):
    return jax.shard_map(
        per_device,
        mesh=mesh,
        in_specs=(
            P(("dp", "seq"), None),
            P("dp"),
            P("dp"),
            P("seq", None),
            P("seq", None),
            P("seq", None),
            P(None, "seq"),
        ),
        out_specs=P(("dp", "seq"), None),
        check_vma=False,
    )
```

```python
import functools

import jax
import jax.numpy as jnp
from jax import lax
from jax.experimental import pallas as pl
from jax.experimental.pallas import tpu as pltpu
from jax.sharding import PartitionSpec as P

HEADS = 8
KV_HEADS = 2
HEAD_DIM = 128
MOST_OWN = 256
ONES = 16
TILES = 4
ADD_TILES = 4
MAIN_VMEM = 36
ADD_VMEM = 12
Q_SHARE = 9
O_SHARE = 18
PLAN = (
    ("W", "oz", 0, 0), ("W", "ox", 0, 0), ("Q", "ox", 0, 0), ("Q", "oz", 0, 0), ("gather",),
    ("W", "x", 0, 1), ("W", "ys", 0, 1), ("W", "z", 1, 0), ("W", "xe", 0, 0), ("W", "ys", 1, 0),
    ("W", "z", 2, 0), ("O", "ox", 0, 0), ("W", "ys", 2, 0), ("O", "oz", 0, 0), ("Q", "x", 0, 1),
    ("Q", "ys", 0, 1), ("W", "x", 1, 1), ("W", "ys", 1, 1), ("W", "z", 3, 0), ("gates", 0),
    ("W", "ys", 3, 0), ("W", "y", 1, 0), ("gates", 2), ("Q", "z", 1, 0), ("W", "y", 2, 0),
    ("W", "x", 2, 1), ("Q", "ys", 1, 0), ("W", "y", 0, 1), ("W", "ys", 2, 1), ("Q", "z", 2, 0),
    ("W", "y", 1, 1), ("W", "e", 2, 0), ("W", "x", 3, 1), ("O", "z", 1, 0), ("W", "ys", 3, 1),
    ("O", "z", 2, 0), ("O", "ys", 2, 0), ("Q", "x", 1, 1), ("Q", "ys", 2, 0), ("W", "y", 3, 0),
    ("Q", "z", 3, 0), ("W", "e", 1, 1), ("W", "e", 1, 0), ("W", "e", 3, 0), ("Q", "ys", 1, 1),
    ("W", "y", 2, 1), ("Q", "x", 2, 1), ("Q", "xe", 0, 0), ("W", "y", 3, 1), ("W", "e", 2, 1),
    ("O", "z", 3, 0), ("Q", "y", 1, 0), ("W", "e", 3, 1), ("W", "e", 0, 1), ("kv",),
    ("Q", "ys", 2, 1), ("K", "z", 0, 0, 1), ("O", "ys", 1, 0), ("K", "z", 0, 0, 0),
    ("Q", "ys", 3, 0), ("O", "x", 0, 1), ("O", "y", 2, 0), ("Q", "y", 1, 1), ("O", "e", 2, 0),
    ("Q", "x", 3, 1), ("Q", "y", 2, 0), ("Q", "ys", 3, 1), ("O", "x", 2, 1), ("O", "x", 1, 1),
    ("K", "z", 1, 0, 1), ("Q", "e", 1, 1), ("gates", 1), ("K", "z", 1, 0, 0), ("O", "ys", 2, 1),
    ("Q", "e", 2, 0), ("O", "ys", 3, 0), ("Q", "y", 3, 0), ("Q", "e", 1, 0), ("O", "ys", 0, 1),
    ("Q", "y", 0, 1), ("O", "y", 1, 0), ("O", "ys", 1, 1), ("K", "x", 0, 1, 1), ("K", "z", 2, 0, 1),
    ("Q", "e", 3, 0), ("O", "xe", 0, 0), ("O", "x", 3, 1), ("Q", "e", 0, 1), ("gates", 3),
    ("O", "e", 1, 0), ("O", "ys", 3, 1), ("Q", "y", 2, 1), ("Q", "y", 3, 1), ("K", "z", 2, 0, 0),
    ("Q", "e", 3, 1), ("Q", "e", 2, 1), ("K", "x", 0, 1, 0), ("q",), ("own",), ("O", "y", 2, 1),
    ("K", "z", 3, 0, 1), ("att", 0, 1), ("att", 2, 0), ("K", "x", 1, 1, 1), ("K", "z", 3, 0, 0),
    ("O", "y", 0, 1), ("O", "y", 3, 0), ("att", 3, 0), ("att", 1, 0), ("K", "x", 1, 1, 0),
    ("O", "y", 1, 1), ("O", "e", 2, 1), ("O", "e", 0, 1), ("O", "e", 3, 0), ("K", "x", 3, 1, 1),
    ("K", "x", 2, 1, 1), ("att", 1, 1), ("K", "x", 2, 1, 0), ("O", "e", 1, 1), ("att", 2, 1),
    ("O", "y", 3, 1), ("K", "x", 3, 1, 0), ("att", 3, 1), ("norm",), ("out", 0, 0), ("out", 3, 0),
    ("out", 0, 1), ("out", 2, 1), ("O", "e", 3, 1), ("out", 1, 0), ("out", 3, 1), ("out", 2, 0),
    ("out", 1, 1),
)
MESH = pl.DeviceIdType.MESH
NEG = -1e30
F32 = jnp.float32
BF16 = jnp.bfloat16


class Ring:
    def __init__(self, geo, sems, region_in, region_y, taken, each=False):
        self.g = geo
        self.sems = sems
        self.region_in = region_in
        self.region_y = region_y
        self.sends = []
        self.some = []
        self.taken = taken
        self.asked = 0
        self.each = each
        self.whole = geo["B"] == 2
        a_count, b_count = geo["A"], geo["B"]
        self.order = arrivals(a_count, b_count)

    def piece(self, k, j):
        g = self.g
        b = lax.rem(g["b"] - j + g["B"], g["B"])
        return at_row(g, lambda row: by_distance(g["A"], row)[k]) * g["B"] + b

    def copy(self, kind, index, ref, dp, seq):
        return remote(ref, self.sems["sent"].at[0], self.sems[kind].at[index], dp, seq)

    def send(self, *args):
        made = self.copy(*args)
        made.start()
        self.sends.append(made)

    def arrive(self, kind, index, ref):
        self.copy(kind, index, ref, self.g["dp"], self.g["x_next"]).wait_recv()

    def mine(self, s):
        return self.region_in(s, self.g["y"], self.g["c"])

    def core_at(self, k, j):
        return self.order.index((k, j)) if self.each else 0

    def send_core(self, k, j):
        g = self.g
        self.send("d", self.core_at(k, j), self.mine(self.piece(k, j)), g["dp_c"], g["seq"])

    def send_y(self, k, j):
        g = self.g
        ref = self.region_y(self.piece(k, j), g["y"], g["c"])
        args = ("y", self.order.index((k, j)), ref, g["dp_y"], g["seq"])
        if self.whole and (k, j) == (0, 1):
            self.send_if(g["a"] > 0, *args)
        else:
            self.send(*args)

    def send_rest(self):
        g = self.g
        if self.whole:
            ref = self.region_y(self.piece(0, 0), 1 - g["y"], g["c"])
            self.send_if(g["a"] == 0, "r", 0, ref, g["dp"], g["x_next"])

    def send_if(self, cond, *args):
        made = self.copy(*args)
        pl.when(cond)(made.start)
        self.some.append((cond, made))

    def send_z(self):
        g = self.g
        mine = self.mine(self.piece(0, 0))
        self.send_if(g["a"] < g["A"] - 1, "u", 0, mine, g["dp"], g["z_up"])
        self.send_if(g["a"] > 0, "v", 0, mine, g["dp"], g["z_down"])

    def take_z(self, k):
        g = self.g
        mine = self.mine(self.piece(k, 0))
        for far in range(1, g["A"]):
            for kind, sign, to in (("u", -1, g["z_up"]), ("v", 1, g["z_down"])):
                rows = [
                    row
                    for row in range(g["A"])
                    if by_distance(g["A"], row)[k] == row + sign * far
                ]
                if not rows:
                    continue
                here = any_row(g, rows)
                pl.when(here)(self.copy(kind, far - 1, mine, g["dp"], to).wait_recv)
                onward = [row for row in rows if 0 <= row - sign < g["A"]]
                if onward:
                    self.send_if(any_row(g, onward), kind, far, mine, g["dp"], to)

    def send_x(self, k):
        g = self.g
        if g["B"] > 1:
            ref = self.mine(self.piece(k, 0))
            self.send("x", k * (g["B"] - 1), ref, g["dp"], g["x_next"])

    def slow(self, k):
        self.take_z(k)
        self.send_x(k)
        self.send_core(k, 0)

    def fast(self, k, j):
        g = self.g
        s = self.piece(k, j)
        self.arrive("x", k * (g["B"] - 1) + j - 1, self.mine(s))
        if j < g["B"] - 1:
            self.send("x", k * (g["B"] - 1) + j, self.mine(s), g["dp"], g["x_next"])
        self.send_core(k, j)

    def relay(self, k, j):
        g = self.g
        index = self.order.index((k, j))
        ref = self.region_y(self.piece(k, j), 1 - g["y"], g["c"])
        if self.whole and (k, j) == (0, 1):
            rest = self.copy("r", 0, ref, g["dp"], g["x_next"])
            over = self.copy("y", index, ref, g["dp_y"], g["seq"])
            pl.when(g["a"] == 0)(rest.wait_recv)
            pl.when(g["a"] > 0)(over.wait_recv)
        else:
            self.arrive("y", index, ref)
        self.send("d", self.core_at(k, j), ref, g["dp_c"], g["seq"])

    def from_core(self, k, j):
        g = self.g
        if self.each:
            self.arrive("d", self.core_at(k, j), self.taken(self.piece(k, j), 1 - g["c"]))
            return
        self.asked += 1
        if self.asked == len(self.order):
            self.arrive("d", 0, self.taken)

    def finish(self):
        for made in self.sends:
            made.wait_send()
        for cond, made in self.some:
            pl.when(cond)(made.wait_send)


class Causal:
    def __init__(self, geo, sems, ref, parts):
        self.g = geo
        self.sems = sems
        self.ref = ref
        self.parts = parts
        self.sends = []
        self.detour = geo["B"] == 2 and geo["A"] >= 2
        self.last = geo["a"] == geo["A"] - 1

    def has(self, k, j):
        g = self.g
        if k > 0:
            return g["a"] >= k
        return g["b"] >= j

    def copy(self, kind, index, e, s, seq):
        recv = self.sems[kind].at[index * self.parts + e]
        return remote(self.ref(s, e), self.sems["sent"].at[0], recv, self.g["dp"], seq)

    def send(self, cond, *args):
        made = self.copy(*args)
        pl.when(cond)(made.start)
        self.sends.append((cond, made))

    def arrive(self, cond, *args):
        pl.when(cond)(self.copy(*args, self.g["z_up"]).wait_recv)

    def slow(self, k, e):
        g = self.g
        s = piece_of(g, k, 0)
        if k > 0:
            self.arrive(g["a"] >= k, "z", k - 1, e, s)
        if k < g["A"] - 1:
            cond = jnp.logical_and(g["a"] >= k, g["a"] + 1 < g["A"])
            self.send(cond, "z", k, e, s, g["z_up"])
        if g["B"] > 1:
            cond = g["a"] >= k if k > 0 else g["b"] + 1 < g["B"]
            if self.detour and k == 1:
                turned = jnp.logical_and(self.last, g["b"] == 0)
                cond = jnp.logical_and(cond, jnp.logical_not(turned))
            self.send(cond, "x", k * (g["B"] - 1), e, s, g["x_next"])

    def fast(self, k, j, e):
        g = self.g
        s = piece_of(g, k, j)
        index = k * (g["B"] - 1) + j - 1
        has = self.has(k, j)
        if self.detour and k == 1:
            turned = jnp.logical_and(self.last, g["b"] == 1)
            self.arrive(turned, "t", 0, e, s)
            has = jnp.logical_and(has, jnp.logical_not(turned))
        self.arrive(has, "x", index, e, s)
        if self.detour and k == 0:
            cond = jnp.logical_and(g["a"] == g["A"] - 2, g["b"] == 1)
            self.send(cond, "t", 0, e, s, g["z_up"])
        if j < g["B"] - 1:
            cond = self.has(k, j)
            if k == 0:
                cond = jnp.logical_and(cond, g["b"] + 1 < g["B"])
            self.send(cond, "x", index + 1, e, s, g["x_next"])

    def finish(self):
        for cond, made in self.sends:
            pl.when(cond)(made.wait_send)


def remote(ref, send, recv, dp, seq):
    return pltpu.make_async_remote_copy(
        src_ref=ref,
        dst_ref=ref,
        send_sem=send,
        recv_sem=recv,
        device_id=(dp, seq),
        device_id_type=MESH,
    )


def arrivals(a_count, b_count):
    order = []
    for k in range(1, a_count):
        order += [(k, 0)] + [(k - 1, j) for j in range(1, b_count)]
    return order + [(a_count - 1, j) for j in range(1, b_count)]


def by_distance(count, row):
    return sorted(range(count), key=lambda other: (abs(other - row), other))


def at_row(g, value):
    result = value(0)
    for row in range(1, g["A"]):
        result = jnp.where(g["a"] == row, value(row), result)
    return result


def any_row(g, rows):
    result = g["a"] == rows[0]
    for row in rows[1:]:
        result = jnp.logical_or(result, g["a"] == row)
    return result


def piece_of(g, k, j):
    a = lax.rem(g["a"] - k + g["A"], g["A"])
    b = lax.rem(g["b"] - j + g["B"], g["B"])
    return a * g["B"] + b


def plan_of(A, B):
    if (A, B) == (4, 2):
        return PLAN
    order = arrivals(A, B)
    taken = {kj: ("z" if kj[1] == 0 else "x", *kj) for kj in order}
    parts = range(KV_HEADS)
    plan = [("gather",)]
    for what in "WQ":
        plan += [(what, "oz", 0, 0), (what, "ox", 0, 0)]
    for what in "WQ":
        for kj in order:
            plan += [(what, *taken[kj]), (what, "ys", *kj)]
    for what in "O":
        plan += [(what, "oz", 0, 0), (what, "ox", 0, 0)]
    plan += [("W", "y", *kj) for kj in order] + [("W", "e", *kj) for kj in order]
    plan += [("gates", i) for i in range(TILES)] + [("kv",)]
    plan += [("K", "z", 0, 0, e) for e in parts]
    for kj in order[: len(order) // 2]:
        for what in "O":
            plan += [(what, *taken[kj]), (what, "ys", *kj)]
    for what in "Q":
        plan += [(what, "y", *kj) for kj in order] + [(what, "e", *kj) for kj in order]
    plan += [("q",), ("own",)]
    for i, kj in enumerate(order):
        plan += [("K", *taken[kj], e) for e in parts] + [("att", *kj)]
        if i >= len(order) // 2:
            for what in "O":
                plan += [(what, *taken[kj]), (what, "ys", *kj)]
    for what in "O":
        plan += [(what, "y", *kj) for kj in order]
    plan += [("norm",), ("out", 0, 0)]
    for kj in order:
        plan += [(what, "e", *kj) for what in "O"] + [("out", *kj)]
    return plan


def up16(value):
    return (value + 15) // 16 * 16


def main_kernel(
    A, B, tok, ch_in, gates_in, wq, wk, wv, wo, blk, oh_out, gate_out,
    ch, gates, oh, tok_v, kvw, qw, obuf, kv, normed, qt, acc, m_s, counts, att, lsem,
    sent, *sems,
):
    n = A * B
    dp = lax.axis_index("dp")
    seq = lax.axis_index("seq")
    a, b = seq // B, lax.rem(seq, B)
    y, c = lax.rem(dp // 2, 2), lax.rem(dp, 2)
    z_up = lax.rem(a + 1, A) * B + b
    z_down = lax.rem(a + A - 1, A) * B + b
    x_next = a * B + lax.rem(b + 1, B)
    x_prev = a * B + lax.rem(b + B - 1, B)
    dp_y = dp + 2 * (1 - 2 * y)
    dp_c = dp + 1 - 2 * c
    geo = dict(
        A=A, B=B, a=a, b=b, y=y, c=c, dp=dp, seq=seq,
        z_up=z_up, z_down=z_down, x_next=x_next, dp_y=dp_y, dp_c=dp_c,
    )
    t_rows = tok.shape[0]
    width = tok.shape[1]
    k_rows = wq.shape[0]
    q_cols, e_cols = wq.shape[1], wk.shape[1]
    o_rows, o_cols = wo.shape
    group = HEADS // KV_HEADS
    pair = 2 * HEAD_DIM

    rows_here = pl.ds(pl.multiple_of(seq * k_rows, k_rows), k_rows)
    local = []
    for e in range(KV_HEADS):
        cols = pl.ds(e * HEAD_DIM, HEAD_DIM)
        local.append((wk.at[:, cols], kvw.at[rows_here, pl.ds(e * pair, HEAD_DIM)]))
        local.append((wv.at[:, cols], kvw.at[rows_here, pl.ds(e * pair + HEAD_DIM, HEAD_DIM)]))
    local += [(wq, qw.at[rows_here, :]), (ch_in, ch), (tok, tok_v), (wo, obuf.at[seq])]
    local += [(gates_in, gates)]
    local = [pltpu.make_async_copy(s, d, lsem.at[i]) for i, (s, d) in enumerate(local)]
    for made in local:
        made.start()
    load_kv, rest = local[: 2 * KV_HEADS], local[2 * KV_HEADS :]
    load_q, load_ch, load_tok, load_o, load_gates = rest

    greet = [(dp_y, seq), (dp_c, seq)]
    if B > 1:
        greet += [(dp, x_next)] + ([(dp, x_prev)] if B > 2 else [])
    barrier = pltpu.get_barrier_semaphore()

    def hail(who):
        pl.semaphore_signal(barrier, inc=1, device_id=who, device_id_type=MESH)

    for who in greet:
        hail(who)
    if A > 1:
        inner = jnp.logical_and(a > 0, a < A - 1)
        pl.when(a < A - 1)(lambda: hail((dp, z_up)))
        pl.when(a > 0)(lambda: hail((dp, z_down)))
        pl.when(inner)(lambda: pl.semaphore_wait(barrier, len(greet) + 2))
        pl.when(jnp.logical_not(inner))(lambda: pl.semaphore_wait(barrier, len(greet) + 1))
    else:
        pl.semaphore_wait(barrier, len(greet))

    quarter = 2 * e_cols // 4

    def w_region(s, y, c):
        return kvw.at[
            pl.ds(pl.multiple_of(s * k_rows, k_rows), k_rows),
            pl.ds(pl.multiple_of((2 * c + y) * quarter, 128), quarter),
        ]

    q_half = q_cols // 2
    q_in = up16(k_rows * Q_SHARE // 16)

    def q_region(s, c, start, size):
        return qw.at[
            pl.ds(pl.multiple_of(s * k_rows + start, 16), size),
            pl.ds(pl.multiple_of(c * q_half, 128), q_half),
        ]

    o_half = o_rows // 2
    o_in = up16(o_half * O_SHARE // 32)

    def o_region(s, start, size):
        return obuf.at[s, pl.ds(pl.multiple_of(start, 16), size), :]

    w_sems, q_sems, o_sems = (
        dict(zip("uvxydr", sems[6 * i : 6 * i + 6]), sent=sent) for i in range(3)
    )
    kz, kx, kt = sems[18:]
    others = pl.ds(0, (n - 1) * k_rows)
    W = Ring(geo, w_sems, w_region, w_region, kvw.at[others, pl.ds(0, 2 * quarter)])
    Q = Ring(
        geo,
        q_sems,
        lambda s, y, c: q_region(s, c, y * (k_rows - q_in), q_in),
        lambda s, y, c: q_region(s, c, y * q_in, k_rows - q_in),
        qw.at[others, pl.ds(0, q_half)],
    )
    O = Ring(
        geo,
        o_sems,
        lambda s, y, c: o_region(s, c * o_half + y * (o_half - o_in), o_in),
        lambda s, y, c: o_region(s, c * o_half + y * o_in, o_half - o_in),
        lambda s, c: o_region(s, c * o_half, o_half),
        each=True,
    )
    rings = {"W": W, "Q": Q, "O": O}
    loads = {"W": load_kv, "Q": [load_q], "O": [load_o]}
    K = Causal(geo, {"z": kz, "x": kx, "t": kt, "sent": sent}, lambda s, e: kv.at[s, e], KV_HEADS)

    def gather():
        load_ch.wait()
        load_gates.wait()
        base = seq * t_rows
        picks = ch[...]
        start = jnp.sum((picks < base).astype(F32), axis=1, keepdims=True)
        rel = picks - base
        inside = (rel >= 0) & (rel < t_rows)
        place = jnp.where(inside, (rel + 1).astype(F32), 0.0)
        rank = lax.broadcasted_iota(jnp.int32, picks.shape, 1).astype(F32) - start
        slots = lax.broadcasted_iota(jnp.int32, (MOST_OWN, 1), 0).astype(F32)
        own = jnp.sum(jnp.where(rank == slots, place, 0.0), axis=1, keepdims=True) - 1.0
        spots = lax.broadcasted_iota(jnp.int32, (1, t_rows), 1).astype(F32)
        oh[...] = (own == spots).astype(F32)
        for t in range(n):
            held = (picks >= t * t_rows) & (picks < (t + 1) * t_rows)
            count = jnp.sum(held.astype(F32), axis=1, keepdims=True)
            counts[t] = jnp.broadcast_to(count, (1, HEAD_DIM))
        load_tok.wait()
        hot = oh[...].astype(BF16)
        chunk = 512
        square = jnp.zeros((MOST_OWN, 1), F32)
        for i in range(width // chunk):
            cols = slice(i * chunk, (i + 1) * chunk)
            rows = jnp.dot(hot, tok_v[:, cols], preferred_element_type=F32)
            square = square + jnp.sum(rows * rows, axis=1, keepdims=True)
            normed[:, cols] = rows.astype(BF16)
        scale = lax.rsqrt(square / width + 1e-06)
        for i in range(width // chunk):
            cols = slice(i * chunk, (i + 1) * chunk)
            normed[:, cols] = (normed[:, cols].astype(F32) * scale).astype(BF16)

    def place_gates(i):
        tile = t_rows // TILES
        low = i * tile
        oh_out[low : low + tile, :] = oh[:, low : low + tile].T.astype(BF16)
        spot = lax.broadcasted_iota(jnp.int32, (tile, 1), 0) + (seq * t_rows + low)
        gate = jnp.sum(jnp.where(ch[...] == spot, gates[...], 0.0), axis=1, keepdims=True)
        gate_out[low : low + tile, :] = jnp.broadcast_to(gate, (tile, HEAD_DIM))

    def project_kv():
        for e in range(KV_HEADS):
            part = jnp.dot(
                normed[...], kvw[:, e * pair : (e + 1) * pair], preferred_element_type=F32
            )
            kv[seq, e, 0] = part[:, :HEAD_DIM].astype(BF16)
            flip = part[:, HEAD_DIM:].T.astype(BF16)
            kv[seq, e, 1, :HEAD_DIM, :] = flip[:, :HEAD_DIM]
            kv[seq, e, 1, HEAD_DIM:, :] = flip[:, HEAD_DIM:]

    def project_q():
        for i in range(HEADS // 2):
            part = jnp.dot(
                normed[...], qw[:, i * pair : (i + 1) * pair], preferred_element_type=F32
            )
            part = part * HEAD_DIM**-0.5
            for h in range(2):
                head = i * 2 + h
                e, first = head // group, (head % group) * MOST_OWN
                flip = part[:, h * HEAD_DIM : (h + 1) * HEAD_DIM].T.astype(BF16)
                qt[e, :HEAD_DIM, first : first + MOST_OWN] = flip
        row = lax.broadcasted_iota(jnp.int32, (HEAD_DIM, group * MOST_OWN), 0)
        for e in range(KV_HEADS):
            qt[e, HEAD_DIM:, :] = (row == 0).astype(F32).astype(BF16)

    def attend(t, diagonal):
        row = lax.broadcasted_iota(jnp.int32, (MOST_OWN, HEAD_DIM), 0).astype(F32)
        bias = jnp.where(row < counts[t], 0.0, NEG).astype(BF16)
        ones = jnp.ones((ONES, MOST_OWN), BF16)
        heads = range(HEADS)
        left, right = [], []
        for e in range(KV_HEADS):
            left.append(jnp.concatenate([kv[t, e, 0], bias], axis=1))
            flip = [kv[t, e, 1, :HEAD_DIM, :], kv[t, e, 1, HEAD_DIM:, :]]
            right.append(jnp.concatenate([jnp.concatenate(flip, axis=1), ones], axis=0))
        score = []
        for f in heads:
            first = (f % group) * MOST_OWN
            query = qt[f // group, :, first : first + MOST_OWN]
            score.append(jnp.dot(left[f // group], query, preferred_element_type=F32))
        if diagonal:
            key = lax.broadcasted_iota(jnp.int32, (MOST_OWN, MOST_OWN), 0)
            asks = lax.broadcasted_iota(jnp.int32, (MOST_OWN, MOST_OWN), 1)
            score = [jnp.where(key <= asks, s, NEG) for s in score]
            top = [jnp.max(s, axis=0, keepdims=True) for s in score]
        else:
            old = [m_s[f] for f in heads]
            held = [acc[f] for f in heads]
            top = [
                jnp.maximum(o, jnp.max(s, axis=0, keepdims=True)) for o, s in zip(old, score)
            ]
        prob = [jnp.exp(s - m).astype(BF16) for s, m in zip(score, top)]
        new = [
            jnp.dot(right[f // group], prob[f], preferred_element_type=F32) for f in heads
        ]
        if not diagonal:
            new = [h * jnp.exp(o - m) + v for h, o, m, v in zip(held, old, top, new)]
        for f in heads:
            m_s[f] = top[f]
            acc[f] = new[f]

    def attend_past(k, j):
        pl.when(K.has(k, j))(lambda: attend(piece_of(geo, k, j), False))

    def finish_attention():
        for f in range(HEADS):
            total = acc[f]
            flip = (total[:HEAD_DIM] / total[HEAD_DIM : HEAD_DIM + 1]).T
            att[:, f * HEAD_DIM : (f + 1) * HEAD_DIM] = flip.astype(BF16)

    def project_out(k, j):
        if o_cols % 128 == 0:
            s = W.piece(k, j)
            cols = pl.ds(pl.multiple_of(s * o_cols, o_cols), o_cols)
            blk[:, cols] = jnp.dot(
                att[...], obuf[s], preferred_element_type=F32
            ).astype(BF16)

    tasks = {
        "gather": gather,
        "gates": place_gates,
        "kv": project_kv,
        "q": project_q,
        "own": lambda: attend(seq, True),
        "att": attend_past,
        "norm": finish_attention,
        "out": project_out,
    }
    for what, *at in plan_of(A, B):
        if what in tasks:
            tasks[what](*at)
            continue
        if what == "K":
            kind, k, j, e = at
            if kind == "z":
                K.slow(k, e)
            else:
                K.fast(k, j, e)
            continue
        ring = rings[what]
        kind, k, j = at
        if kind in ("oz", "ox", "xe"):
            for made in loads[what]:
                made.wait()
            loads[what] = []
        if kind == "oz":
            ring.send_z()
        elif kind == "ox":
            ring.send_x(0)
        elif kind == "xe":
            ring.send_rest()
        elif kind == "z":
            ring.slow(k)
        elif kind == "x":
            ring.fast(k, j)
        elif kind == "ys":
            ring.send_y(k, j)
        elif kind == "y":
            ring.relay(k, j)
        else:
            ring.from_core(k, j)
    if o_cols % 128 != 0:
        for s in range(n):
            blk[:, s * o_cols : (s + 1) * o_cols] = jnp.dot(
                att[...], obuf[s], preferred_element_type=F32
            ).astype(BF16)
    for ring in (*rings.values(), K):
        ring.finish()


def add_kernel(tok, gate, oh, blk, out, made, sems):
    tile = tok.shape[0] // ADD_TILES
    copies = []
    for i in range(ADD_TILES):
        rows = pl.ds(i * tile, tile)
        for first in range(0, tok.shape[1], 2 * HEAD_DIM):
            right = blk[:, first : first + 2 * HEAD_DIM]
            lift = jnp.dot(oh[rows, :], right, preferred_element_type=F32)
            for j in range(0, 2 * HEAD_DIM, HEAD_DIM):
                cols = slice(first + j, first + j + HEAD_DIM)
                added = gate[rows, :] * lift[:, j : j + HEAD_DIM]
                made[rows, cols] = (tok[rows, cols].astype(F32) + added).astype(BF16)
        copies.append(pltpu.make_async_copy(made.at[rows], out.at[rows], sems.at[i]))
        copies[-1].start()
    for copy in copies:
        copy.wait()


def in_hbm(array):
    return pltpu.with_memory_space_constraint(array, pltpu.HBM)


def per_device(tokens, chosen, gates, w_query, w_key, w_value, w_out):
    n = lax.axis_size("seq")
    A = 4 if n % 4 == 0 else 1
    B = n // A
    t_rows, width = tokens.shape
    k_rows, q_cols = w_query.shape
    e_cols = w_key.shape[1]
    o_rows, o_cols = w_out.shape
    picks = chosen.reshape(1, -1)
    gate_row = gates.reshape(1, -1)
    dma = pltpu.SemaphoreType.DMA
    hbm_spec = pl.BlockSpec(memory_space=pltpu.HBM)
    vmem_spec = pl.BlockSpec(memory_space=pltpu.VMEM)
    steps_x = max(A * (B - 1), 1)
    steps_z = max(A - 1, 1)

    counts = []
    for cores in (1, 1, n - 1):
        counts += [steps_z, steps_z, steps_x, n - 1, cores, 1]
    counts += [KV_HEADS * steps_z, KV_HEADS * steps_x, KV_HEADS]
    flat = [dma((1,))] + [dma((count,)) for count in counts]

    def body(*refs):
        main_kernel(A, B, *refs)

    blk, oh, gate = pl.pallas_call(
        body,
        out_shape=(
            jax.ShapeDtypeStruct((MOST_OWN, width), BF16),
            jax.ShapeDtypeStruct((t_rows, MOST_OWN), BF16),
            jax.ShapeDtypeStruct((t_rows, HEAD_DIM), F32),
        ),
        in_specs=[hbm_spec] * 7,
        out_specs=(vmem_spec, vmem_spec, vmem_spec),
        scratch_shapes=[
            pltpu.VMEM(picks.shape, jnp.int32),
            pltpu.VMEM(picks.shape, F32),
            pltpu.VMEM((MOST_OWN, t_rows), F32),
            pltpu.VMEM((t_rows, width), BF16),
            pltpu.VMEM((n * k_rows, 2 * e_cols), BF16),
            pltpu.VMEM((n * k_rows, q_cols), BF16),
            pltpu.VMEM((n, o_rows, o_cols), BF16),
            pltpu.VMEM((n, KV_HEADS, 2, MOST_OWN, HEAD_DIM), BF16),
            pltpu.VMEM((MOST_OWN, width), BF16),
            pltpu.VMEM((KV_HEADS, 2 * HEAD_DIM, HEADS // KV_HEADS * MOST_OWN), BF16),
            pltpu.VMEM((HEADS, HEAD_DIM + ONES, MOST_OWN), F32),
            pltpu.VMEM((HEADS, 1, MOST_OWN), F32),
            pltpu.VMEM((n, 1, HEAD_DIM), F32),
            pltpu.VMEM((MOST_OWN, HEADS * HEAD_DIM), BF16),
            dma((2 * KV_HEADS + 5,)),
            *flat,
        ],
        compiler_params=pltpu.CompilerParams(
            collective_id=0, has_side_effects=True, vmem_limit_bytes=MAIN_VMEM * 1024 * 1024
        ),
        name="gather_attend",
    )(
        *map(in_hbm, (tokens, picks, gate_row, w_query, w_key, w_value, w_out))
    )

    return pl.pallas_call(
        add_kernel,
        out_shape=jax.ShapeDtypeStruct((t_rows, width), BF16),
        in_specs=[vmem_spec] * 4,
        out_specs=hbm_spec,
        scratch_shapes=[pltpu.VMEM((t_rows, width), BF16), dma((ADD_TILES,))],
        compiler_params=pltpu.CompilerParams(vmem_limit_bytes=ADD_VMEM * 1024 * 1024),
        name="add_rows",
    )(tokens, gate, oh, blk)


def solution(mesh):
    return jax.shard_map(
        per_device,
        mesh=mesh,
        in_specs=(
            P(("dp", "seq"), None),
            P("dp"),
            P("dp"),
            P("seq", None),
            P("seq", None),
            P("seq", None),
            P(None, "seq"),
        ),
        out_specs=P(("dp", "seq"), None),
        check_vma=False,
    )
```
